16 devices in a mesh: dp: 2 (over y, z), ep: 8 (over x, core).
Axes of the slice: x: 4, y: 2, z: 1, core: 2. Of those that a mesh axis runs over, the one named last changes fastest.
The devices are a block of a 4x4x8 slice.
Arguments:
- tokens: bfloat16 [2048, 2048], P(('dp', 'ep')), parts along dimension 0
- expert_ids: int32 [2048, 8], P(('dp', 'ep')), parts along dimension 0
- norm_gain: bfloat16 [2048], replicated
- w_router: bfloat16 [2048, 64], replicated
- w_gate: bfloat16 [64, 2048, 1024], P('ep')
- w_up: bfloat16 [64, 2048, 1024], P('ep')
- w_down: bfloat16 [64, 1024, 2048], P('ep')
Outputs:
- output: bfloat16 [2048, 2048], P(('dp', 'ep')), parts along dimension 0
There are 2 independent parts. The reference program is written for one: setup_inputs(seed, part) draws one part's arguments, and reference() takes and returns one part's arrays. A program takes and returns all parts, laid end to end along the dimension named above; an argument that names none is the same for every part.
All inputs are finite; a program needn't handle non-finite values.
Results may differ from the reference program's by a relative error of at most 0.00576213.
Values are sent between devices in bfloat16 or wider.
A program may use at most 768 MiB of HBM per device.

```python
import jax
import jax.numpy as jnp
from jax import lax

D = 2048
EXPERTS = 64
TOP = 8
FF = 1024
TOKENS_DEV = 128
EP_SIZE = 8
BLOCK_ROWS = 128

TOKENS = EP_SIZE * TOKENS_DEV
PAIRS = TOKENS * TOP
E_LOCAL = EXPERTS // EP_SIZE
NUM_BLOCKS = PAIRS // BLOCK_ROWS + EXPERTS + 1
NORM_EPS = 1e-5


def draw_routes(route_key):
    sub_keys = jax.random.split(route_key, 6)
    pair_dev = TOKENS_DEV * TOP
    half_mean = pair_dev // (2 * EP_SIZE)
    hot_dev = jax.random.randint(sub_keys[0], (), 0, EP_SIZE)
    rotation = jax.random.randint(sub_keys[1], (), 0, EP_SIZE - 1)
    rest_weight = jax.random.randint(sub_keys[2], (EP_SIZE - 2,), 1, 3)
    rest_cum = jnp.concatenate([jnp.zeros((1,), jnp.int32), jnp.cumsum(rest_weight)])
    rest_bound = (pair_dev - 7 * half_mean) * rest_cum // rest_cum[-1]
    pattern = jnp.concatenate([jnp.full((1,), 4 * half_mean, jnp.int32), rest_bound[1:] - rest_bound[:-1]])
    src_dev = jnp.arange(EP_SIZE)[:, None]
    dst_dev = jnp.arange(EP_SIZE)[None, :]
    shift_idx = ((dst_dev - hot_dev - 1) % EP_SIZE - src_dev - rotation) % (EP_SIZE - 1)
    dev_load = jnp.where(dst_dev == hot_dev, 3 * half_mean, pattern[shift_idx])
    split_weight = jax.random.randint(sub_keys[3], (EP_SIZE, EP_SIZE, E_LOCAL), 1, 4)
    split_cum = jnp.concatenate([jnp.zeros((EP_SIZE, EP_SIZE, 1), jnp.int32), jnp.cumsum(split_weight, axis=2)], axis=2)
    split_bound = dev_load[:, :, None] * split_cum // split_cum[:, :, -1:]
    expert_count = (split_bound[:, :, 1:] - split_bound[:, :, :-1]).reshape(EP_SIZE, EXPERTS)
    count_end = jnp.cumsum(expert_count, axis=1)
    positions = jnp.arange(pair_dev)
    sorted_ids = jax.vmap(lambda end_row: jnp.searchsorted(end_row, positions, side='right'))(count_end)
    by_token = sorted_ids.reshape(EP_SIZE, TOP, TOKENS_DEV).transpose(0, 2, 1)
    tok_perm = jax.vmap(lambda perm_key: jax.random.permutation(perm_key, TOKENS_DEV))(jax.random.split(sub_keys[4], EP_SIZE))
    by_token = jnp.take_along_axis(by_token, jnp.broadcast_to(tok_perm[:, :, None], (EP_SIZE, TOKENS_DEV, TOP)), axis=1)
    turn = jax.random.randint(sub_keys[5], (EP_SIZE, TOKENS_DEV, 1), 0, TOP)
    col_idx = (jnp.arange(TOP)[None, None, :] + turn) % TOP
    by_token = jnp.take_along_axis(by_token, col_idx, axis=2)
    return by_token.reshape(TOKENS, TOP).astype(jnp.int32)


def setup_inputs(seed: int = 0, part: int = 0) -> dict:
    part_key = jax.random.fold_in(jax.random.key(seed), part)
    tok_key, route_key = jax.random.split(part_key)
    shared = jax.random.split(jax.random.key(seed + 1), 5)
    tokens = jax.random.normal(tok_key, (TOKENS, D), jnp.float32).astype(jnp.bfloat16)
    norm_gain = (1.0 + 0.3 * jax.random.normal(shared[0], (D,), jnp.float32)).astype(jnp.bfloat16)
    w_router = (jax.random.normal(shared[1], (D, EXPERTS), jnp.float32) * D ** -0.5).astype(jnp.bfloat16)
    w_gate = (jax.random.normal(shared[2], (EXPERTS, D, FF), jnp.float32) * D ** -0.5).astype(jnp.bfloat16)
    w_up = (jax.random.normal(shared[3], (EXPERTS, D, FF), jnp.float32) * D ** -0.5).astype(jnp.bfloat16)
    w_down = (jax.random.normal(shared[4], (EXPERTS, FF, D), jnp.float32) * (EXPERTS / 4 * FF ** -0.5)).astype(jnp.bfloat16)
    expert_ids = draw_routes(route_key)
    return {'tokens': tokens, 'expert_ids': expert_ids, 'norm_gain': norm_gain, 'w_router': w_router, 'w_gate': w_gate, 'w_up': w_up, 'w_down': w_down}


def reference(tokens, expert_ids, norm_gain, w_router, w_gate, w_up, w_down):
    tok32 = tokens.astype(jnp.float32)
    inv_rms = lax.rsqrt(jnp.mean(tok32 * tok32, axis=1, keepdims=True) + NORM_EPS)
    normed = (tok32 * inv_rms * norm_gain.astype(jnp.float32)).astype(jnp.bfloat16)
    logits = jnp.dot(normed, w_router, preferred_element_type=jnp.float32)
    router_prob = jax.nn.softmax(logits, axis=1)
    gate_vals = jnp.take_along_axis(router_prob, expert_ids, axis=1)
    flat_ids = expert_ids.reshape(PAIRS)
    sort_order = jnp.argsort(flat_ids, stable=True)
    sorted_ids = flat_ids[sort_order]
    counts = jnp.bincount(flat_ids, length=EXPERTS)
    padded = (counts + BLOCK_ROWS - 1) // BLOCK_ROWS * BLOCK_ROWS
    pad_end = jnp.cumsum(padded)
    group_start = jnp.cumsum(counts) - counts
    slot_sorted = pad_end[sorted_ids] - padded[sorted_ids] + jnp.arange(PAIRS) - group_start[sorted_ids]
    row_buf = jnp.zeros((NUM_BLOCKS * BLOCK_ROWS, D), jnp.bfloat16).at[slot_sorted].set(normed[sort_order // TOP])
    block_expert = jnp.minimum(jnp.searchsorted(pad_end, jnp.arange(NUM_BLOCKS) * BLOCK_ROWS, side='right'), EXPERTS - 1)

    def block_apply(block_args):
        block_rows, expert = block_args
        hidden_gate = jnp.dot(block_rows, w_gate[expert], preferred_element_type=jnp.float32)
        hidden_up = jnp.dot(block_rows, w_up[expert], preferred_element_type=jnp.float32)
        swiglu_out = (jax.nn.silu(hidden_gate) * hidden_up).astype(jnp.bfloat16)
        return jnp.dot(swiglu_out, w_down[expert], preferred_element_type=jnp.float32).astype(jnp.bfloat16)

    block_out = lax.map(block_apply, (row_buf.reshape(NUM_BLOCKS, BLOCK_ROWS, D), block_expert))
    slot_pair = jnp.zeros((PAIRS,), jnp.int32).at[sort_order].set(slot_sorted)
    pair_out = block_out.reshape(NUM_BLOCKS * BLOCK_ROWS, D)[slot_pair].reshape(TOKENS, TOP, D)
    moe_sum = jnp.einsum('nk,nkd->nd', gate_vals, pair_out.astype(jnp.float32))
    return (tok32 + moe_sum).astype(jnp.bfloat16)
```

```python
import functools

import jax
import jax.numpy as jnp
from jax import lax
from jax.experimental import pallas as pl
from jax.experimental.pallas import tpu as pltpu
from jax.sharding import PartitionSpec as P

NORM_EPS = 1e-5
TILE = 128
SUB = 8
LANE = 128
F32 = jnp.float32
BF16 = jnp.bfloat16
MESH = pl.DeviceIdType.MESH


def dot(a, b, dims=(((1,), (0,)), ((), ()))):
    return lax.dot_general(a, b, dims, preferred_element_type=F32)


NT_DIMS = (((1,), (1,)), ((), ()))


class Place:
    def __init__(self, ep):
        self.ep = ep
        self.me = lax.axis_index("ep")
        self.xi, self.core = self.me // 2, self.me % 2
        self.chips = ep // 2
        self.right, self.left, self.far = self.dev(1, self.core), self.dev(-1, self.core), self.dev(2, self.core)
        self.partner = self.dev(0, 1 - self.core)

    def dev(self, dx, c):
        return lax.rem(self.xi + dx + self.chips, self.chips) * 2 + c

    def signal_all(self):
        barrier = pltpu.get_barrier_semaphore()
        for d in range(1, self.ep):
            pl.semaphore_signal(barrier, inc=1, device_id={"ep": lax.rem(self.me + d, self.ep)}, device_id_type=MESH)
        return barrier


class Gather:
    def __init__(self, pc, ref, send, recv, tok, own=None):
        self.pc, self.ref, self.send, self.recv, self.tok, self.own = pc, ref, send, recv, tok, own

    def copy(self, j, block, r, target, own=False):
        hr = self.tok // 2
        rows = pl.ds(pl.multiple_of(block * self.tok + r * hr, hr), hr)
        dst = self.ref.at[rows, :]
        src = self.own.at[pl.ds(r * hr, hr), :] if own and self.own is not None else dst
        return pltpu.make_async_remote_copy(
            src, dst, self.send.at[j], self.recv.at[j], device_id={"ep": target}, device_id_type=MESH)

    def start(self):
        p = self.pc
        self.copy(0, p.me, 0, p.right, True).start()
        self.copy(2, p.me, 1, p.left, True).start()
        self.copy(1, p.me, 1, p.right, True).start()
        self.copy(3, p.me, 0, p.left, True).start()
        self.copy(6, p.me, 0, p.partner, True).start()
        self.copy(7, p.me, 1, p.partner, True).start()

    def forward(self):
        p = self.pc
        self.copy(0, p.left, 0, p.right).wait_recv()
        self.copy(4, p.left, 0, p.right).start()
        self.copy(8, p.left, 0, p.partner).start()
        self.copy(2, p.right, 1, p.left).wait_recv()
        self.copy(5, p.right, 1, p.left).start()
        self.copy(11, p.right, 1, p.partner).start()

    def rest(self):
        p = self.pc
        self.copy(1, p.left, 1, p.right).wait_recv()
        self.copy(9, p.left, 1, p.partner).start()
        self.copy(3, p.right, 0, p.left).wait_recv()
        self.copy(10, p.right, 0, p.partner).start()

    def last(self):
        p = self.pc
        self.copy(4, p.far, 0, p.right).wait_recv()
        self.copy(12, p.far, 0, p.partner).start()
        self.copy(5, p.far, 1, p.left).wait_recv()
        self.copy(13, p.far, 1, p.partner).start()

    def finish(self):
        p = self.pc
        for j, (dx, r) in enumerate(((0, 0), (0, 1), (-1, 0), (-1, 1), (1, 0), (1, 1), (2, 0), (2, 1))):
            self.copy(6 + j, p.dev(dx, 1 - p.core), r, p.partner).wait_recv()

    def drain(self):
        for j in range(14):
            self.copy(j, self.pc.me, 0, self.pc.right).wait_send()


def plan_kernel(
    ep, tiles,
    x_ref, ids_ref, gain_ref, wr_ref,
    u0_ref, u1_ref, slot_ref, src_v, first_v, last_v, te_v, gate_v,
    p_ref, id_land, p_land,
    small_send, small_recv, ag_send, ag_recv,
):
    pc = Place(ep)
    me = pc.me
    tok, width = x_ref.shape
    half_w = width // 2
    e_local = slot_ref.shape[0]
    q_max = src_v.shape[1]
    barrier = pc.signal_all()

    x32 = x_ref[...].astype(F32)
    inv = lax.rsqrt(jnp.mean(x32 * x32, axis=1, keepdims=True) + NORM_EPS)
    u_own = (x32 * inv * gain_ref[...].astype(F32)).astype(BF16)
    own_rows = pl.ds(pl.multiple_of(me * tok, tok), tok)
    u0_ref[own_rows, :] = u_own[:, :half_w]
    u1_ref[...] = u_own[:, half_w:]

    pl.semaphore_wait(barrier, ep - 1)

    ag = Gather(pc, u0_ref, ag_send, ag_recv, tok)
    ag.start()

    logits = dot(u_own, wr_ref[...])
    n_exp = logits.shape[1]
    logits = jnp.concatenate([logits, jnp.zeros((tok, LANE - n_exp), F32)], axis=1).T[:n_exp]
    ex = jnp.exp(logits - jnp.max(logits, axis=0, keepdims=True))
    p_ref[...] = ex / jnp.sum(ex, axis=0, keepdims=True)
    id_land[me] = ids_ref[...]
    p_land[me] = p_ref[pl.ds(pl.multiple_of(me * e_local, e_local), e_local), :]

    def small(d, kind, target):
        if kind == 0:
            src, dst = ids_ref, id_land.at[me]
        else:
            src, dst = p_ref.at[pl.ds(pl.multiple_of(target * e_local, e_local), e_local), :], p_land.at[me]
        return pltpu.make_async_remote_copy(
            src, dst, small_send.at[kind, d], small_recv.at[kind, d], device_id={"ep": target}, device_id_type=MESH)

    for kind in range(2):
        for d in range(1, ep):
            small(d, kind, lax.rem(me + d, ep)).start()
    for kind in range(2):
        for d in range(1, ep):
            small(d, kind, lax.rem(me + d, ep)).wait_recv()

    base = me * e_local
    sub_i = lax.broadcasted_iota(jnp.int32, (e_local, LANE), 0)
    lane_i = lax.broadcasted_iota(jnp.int32, (e_local, LANE), 1)
    tri = (lax.broadcasted_iota(jnp.int32, (LANE, LANE), 0) < lax.broadcasted_iota(jnp.int32, (LANE, LANE), 1)).astype(BF16)
    member = []
    for b in range(ep):
        ids_b = id_land[b]
        m = jnp.zeros((e_local, LANE), F32)
        for k in range(ids_b.shape[0]):
            m = m + jnp.where(ids_b[k:k + 1, :] == base + sub_i, 1.0, 0.0)
        member.append(m)
    stack = jnp.concatenate(member, axis=0)
    before = dot(stack.astype(BF16), tri)
    total = jnp.sum(stack, axis=1, keepdims=True)
    run = jnp.zeros((e_local, 1), F32)
    pos = []
    for b in range(ep):
        pos.append(before[b * e_local:(b + 1) * e_local] + run)
        run = run + total[b * e_local:(b + 1) * e_local]
    tiles_e = jnp.floor((run + (TILE - 1)) * (1.0 / TILE))
    start = jnp.zeros((e_local, 1), F32)
    sub_c = lax.broadcasted_iota(jnp.int32, (e_local, 1), 0)
    for e in range(e_local):
        start = start + jnp.where(sub_c > e, tiles_e[e:e + 1, :], 0.0)
    tile_end = start + tiles_e
    te = jnp.sum(jnp.where(tile_end <= lane_i.astype(F32), 1.0, 0.0), axis=0, keepdims=True)
    te_v[...] = jnp.clip(te.astype(jnp.int32), 0, e_local - 1)
    count = jnp.concatenate([jnp.sum(m, axis=0, keepdims=True) for m in member], axis=0)
    first_rank = dot(count.astype(BF16), tri)
    last_row = jnp.where(count > 0, first_rank + count - 1.0, q_max * 1.0)
    last_v[...] = jnp.clip(last_row.astype(jnp.int32), 0, q_max)
    q_row = lax.broadcasted_iota(jnp.int32, (q_max, LANE), 0).astype(F32)
    q_lane = lax.broadcasted_iota(jnp.int32, (e_local, q_max), 1).astype(F32)
    for b in range(ep):
        m = member[b]
        slot = jnp.where(m > 0, start * TILE + pos[b], -1.0)
        slot_ref[:, :, b * LANE:(b + 1) * LANE] = jnp.broadcast_to(slot[:, None, :], (e_local, SUB, LANE))
        pre = jnp.zeros((e_local, LANE), F32)
        for e in range(e_local):
            pre = pre + jnp.where(sub_i > e, m[e:e + 1, :], 0.0)
        fr, ct = first_rank[b:b + 1], count[b:b + 1]
        rank = jnp.where(m > 0, fr + pre, 300.0)
        hi = jnp.floor(slot * (1.0 / 64))
        pb = p_land[b]
        g1 = pb.astype(BF16).astype(F32)
        g2 = (pb - g1).astype(BF16).astype(F32)
        g3 = pb - g1 - g2
        feats = jnp.concatenate([rank, hi, slot - hi * 64.0, jnp.broadcast_to(fr, m.shape), g1, g2, g3, pre], axis=0)
        hot = jnp.where((q_row >= fr) & (q_row < fr + ct), 1.0, 0.0).astype(BF16)
        got = dot(feats.astype(BF16), hot, NT_DIMS)
        e8 = e_local
        sel = got[0:e8] == q_lane
        src = jnp.sum(jnp.where(sel, got[e8:2 * e8] * 64.0 + got[2 * e8:3 * e8], 0.0), axis=0, keepdims=True)
        gate = jnp.sum(jnp.where(sel, got[4 * e8:5 * e8] + got[5 * e8:6 * e8] + got[6 * e8:7 * e8], 0.0), axis=0, keepdims=True)
        src_v[b:b + 1, :] = jnp.clip(src.astype(jnp.int32), 0, tiles * TILE - 1)
        first_v[b:b + 1, :] = (got[3 * e8:3 * e8 + 1] == q_lane[0:1]).astype(jnp.int32)
        gate_v[b:b + 1, :] = gate

    ag.forward()
    ag.rest()
    ag.last()
    ag.finish()
    ag.drain()
    for kind in range(2):
        for d in range(1, ep):
            small(d, kind, lax.rem(me + d, ep)).wait_send()


def moe_kernel(
    ep, tiles,
    te_s, src_s, first_s, last_s, gate_s,
    u0_hbm, u1_ref, slot_ref, x_hbm, w1_hbm, w3_hbm, w2_hbm,
    out_ref,
    u_all, x_v, h_ref, ring0, ring1, ring2, ring3,
    recv_a, recv_h, recv_d,
    in_sem, ring_sem, ag_send, ag_recv,
    a_send, a_recv, h_send, h_recv, d_send, d_recv,
):
    pc = Place(ep)
    me, core, chips, dev = pc.me, pc.core, pc.chips, pc.dev
    right, left, partner, far = pc.right, pc.left, pc.partner, pc.far
    ring = (ring0, ring1, ring2, ring3)
    tok, width = x_v.shape
    q_max = src_s.shape[1]
    half_w = width // 2
    ff = h_ref.shape[1]
    e_local, _, fcol = ring0.shape
    n_fs = ff // fcol
    rows_blk = tok * SUB

    def w13_copy(m, buf):
        kk, ffi = m // (2 * n_fs), (m % (2 * n_fs)) // 2
        rows = pl.ds(pl.multiple_of(kk * half_w, half_w), half_w)
        cols = pl.ds(pl.multiple_of(ffi * fcol, fcol), fcol)
        return [pltpu.make_async_copy(w.at[:, rows, cols], ring[buf], ring_sem.at[buf]) for w in (w1_hbm, w3_hbm)]

    def w2_copy(cs, buf):
        cols = pl.ds(pl.multiple_of(cs * fcol, fcol), fcol)
        return pltpu.make_async_copy(w2_hbm.at[:, :, cols], ring[buf], ring_sem.at[buf])

    for m in range(4):
        w13_copy(m, m)[m % 2].start()

    barrier = pc.signal_all()

    pltpu.make_async_copy(u0_hbm, u_all.at[0], in_sem.at[0]).start()
    pltpu.make_async_copy(x_hbm, x_v, in_sem.at[1]).start()
    own_rows = pl.ds(pl.multiple_of(me * tok, tok), tok)
    pl.semaphore_wait(barrier, ep - 1)
    ag = Gather(pc, u_all.at[1], ag_send, ag_recv, tok, own=u1_ref)
    ag.start()
    u_all[1, own_rows, :] = u1_ref[...]
    pltpu.make_async_copy(u0_hbm, u_all.at[0], in_sem.at[0]).wait()

    def tile_expert(i):
        return te_s[0, i]

    def phase_one(ug, acc):
        t_iota = lax.broadcasted_iota(jnp.int32, (TILE, ep * tok), 0).astype(F32)

        def gather(k, lo, hi, un):
            def body(g, carry):
                for j in range(un):
                    i = lo + g * un + j
                    row = slot_ref[tile_expert(i)][0:1] - lax.convert_element_type(i * TILE, F32)
                    hot = jnp.where(row == t_iota, 1.0, 0.0).astype(BF16)
                    ug[pl.ds(pl.multiple_of(i * TILE, TILE), TILE), :] = dot(hot, u_all[k]).astype(BF16)
                return carry

            lax.fori_loop(0, (hi - lo) // un, body, 0)

        def units(k):
            def two_units(fp, carry):
                for b1 in (0, 2):
                    fs = 2 * fp + b1 // 2
                    n = k * 2 * n_fs + 2 * fs
                    for which in range(2):
                        w13_copy(n, b1 + which)[which].wait()
                    for which in range(2):
                        for i in range(tiles):
                            rows = pl.ds(i * TILE, TILE)
                            d = dot(ug[rows, :], ring[b1 + which][tile_expert(i)])
                            if k == 0:
                                acc[which, fs, rows, :] = d
                            elif which == 0:
                                acc[0, fs, rows, :] = acc[0, fs, rows, :] + d
                            else:
                                g = acc[0, fs, rows, :]
                                hcols = pl.ds(pl.multiple_of(fs * fcol, fcol), fcol)
                                h_ref[rows, hcols] = (g / (1.0 + jnp.exp(-g)) * (acc[1, fs, rows, :] + d)).astype(BF16)
                        if k == 0:
                            w13_copy(n + 4 + which, b1 + which)[which].start()
                        else:
                            @pl.when(fp == 0)
                            def _():
                                w13_copy(n + 4 + which, b1 + which)[which].start()

                            @pl.when(fp > 0)
                            def _():
                                w2_copy(b1 + which, b1 + which).start()
                return carry

            lax.fori_loop(0, n_fs // 2, two_units, 0)

        mid = tiles // 2
        gather(0, 0, mid, 3)
        ag.forward()
        gather(0, mid, tiles, 5)
        ag.rest()
        units(0)
        ag.last()
        ag.finish()
        gather(1, 0, mid, 3)
        gather(1, mid, tiles, 5)
        units(1)

    pl.run_scoped(
        phase_one,
        pltpu.VMEM((tiles * TILE, half_w), BF16),
        pltpu.VMEM((2, n_fs, tiles * TILE, fcol), F32),
    )

    def phase_two(o3, pbuf, accb):
        n_slice = half_w // fcol
        order = (2, 1, 3, 0)
        o_rows = o3.reshape(o3.shape[0] // SUB, SUB, LANE)
        p_rows = pbuf.reshape(pbuf.shape[0] // SUB, SUB, LANE)
        pbuf[q_max * SUB:(q_max + 1) * SUB, :] = jnp.zeros((SUB, LANE), F32)

        def down(q):
            def body(jp, carry):
                for b1 in range(4):
                    j = jp * 4 + b1
                    w2_copy(q * n_slice + j, b1).wait()
                    for i in range(tiles):
                        o = dot(h_ref[i * TILE:(i + 1) * TILE, :], ring[b1][tile_expert(i)]).astype(BF16).astype(F32)
                        for v in range(fcol // LANE):
                            o3[pl.ds(i * TILE * SUB + j * (fcol // LANE) + v, TILE, stride=SUB), :] = o[:, v * LANE:(v + 1) * LANE]
                    if q == 0:
                        w2_copy(n_slice + j, b1).start()
                return carry

            lax.fori_loop(0, n_slice // 4, body, 0)

        def block(q, s):
            return pl.ds(pl.multiple_of((q * ep + s) * rows_blk, rows_blk), rows_blk)

        def combine(q, s):
            un = 8

            def pairs(i, run):
                for j in range(un):
                    qq = i * un + j
                    row = o_rows[src_s[s, qq]]
                    run = jnp.where(jnp.full((SUB, LANE), first_s[s, qq], jnp.int32) == 1, 0.0, run) + gate_s[s, qq] * row
                    pbuf[pl.ds(pl.multiple_of(qq * SUB, SUB), SUB), :] = run
                return run

            lax.fori_loop(0, q_max // un, pairs, jnp.zeros((SUB, LANE), F32))

            def tokens(i, carry):
                for j in range(un):
                    t = i * un + j
                    dst = pl.ds(pl.multiple_of((q * ep + s) * rows_blk + t * SUB, SUB), SUB)
                    accb[dst, :] = p_rows[last_s[s, t]]
                return carry

            lax.fori_loop(0, tok // un, tokens, 0)

        def a_copy(q, j):
            rows = pl.ds((q * chips + j) * rows_blk, rows_blk)
            return pltpu.make_async_remote_copy(
                accb.at[block(q, dev(order[j], 1 - core)), :], recv_a.at[rows, :], a_send.at[q, j], a_recv.at[q, j],
                device_id={"ep": partner}, device_id_type=MESH)

        def a_add(q, j):
            a_copy(q, j).wait_recv()
            mine = block(q, dev(order[j], core))
            accb[mine, :] = accb[mine, :] + recv_a[(q * chips + j) * rows_blk:(q * chips + j + 1) * rows_blk, :]

        hb = rows_blk // 2

        def half(q, s, r):
            return pl.ds(pl.multiple_of((q * ep + s) * rows_blk + r * hb, hb), hb)

        def h_copy(q, side):
            return pltpu.make_async_remote_copy(
                accb.at[half(q, far, side), :], recv_h.at[pl.ds((q * 2 + side) * hb, hb), :], h_send.at[q, side], h_recv.at[q, side],
                device_id={"ep": left if side else right}, device_id_type=MESH)

        def d_copy(q, side, r):
            s = left if side else right
            return pltpu.make_async_remote_copy(
                accb.at[half(q, s, r), :], recv_d.at[pl.ds((q * 2 + side) * rows_blk + r * hb, hb), :],
                d_send.at[q, side * 2 + r], d_recv.at[q, side * 2 + r], device_id={"ep": s}, device_id_type=MESH)

        def relay(q):
            for side in range(2):
                h_copy(q, side).wait_recv()
                s = left if side else right
                mine = half(q, s, side)
                accb[mine, :] = accb[mine, :] + recv_h[(q * 2 + side) * hb:(q * 2 + side + 1) * hb, :]
                d_copy(q, side, side).start()

        def scatter(q):
            for j in range(chips):
                combine(q, dev(order[j], 1 - core))
                a_copy(q, j).start()
                combine(q, dev(order[j], core))
                a_add(q, j)
                if j == 0:
                    h_copy(q, 0).start()
                    h_copy(q, 1).start()
                elif j == 1:
                    d_copy(q, 0, 1).start()
                elif j == 2:
                    d_copy(q, 1, 0).start()

        def finish(q):
            for side in range(2):
                for r in range(2):
                    d_copy(q, side, r).wait_recv()
            for v in range(half_w // LANE):
                cols = slice(q * half_w + v * LANE, q * half_w + (v + 1) * LANE)
                own = accb[pl.ds((q * ep + me) * rows_blk + v, tok, stride=SUB), :]
                d0 = recv_d[pl.ds(q * 2 * rows_blk + v, tok, stride=SUB), :]
                d1 = recv_d[pl.ds((q * 2 + 1) * rows_blk + v, tok, stride=SUB), :]
                out_ref[:, cols] = (x_v[:, cols].astype(F32) + (own + d0 + d1)).astype(BF16)

        down(0)
        scatter(0)
        down(1)
        relay(0)
        scatter(1)
        relay(1)
        pltpu.make_async_copy(x_hbm, x_v, in_sem.at[1]).wait()
        finish(0)
        finish(1)
        for q in range(2):
            for j in range(chips):
                a_copy(q, j).wait_send()
            for side in range(2):
                h_copy(q, side).wait_send()
                for r in range(2):
                    d_copy(q, side, r).wait_send()

    pl.run_scoped(
        phase_two,
        pltpu.VMEM((tiles * TILE * SUB + SUB, LANE), F32),
        pltpu.VMEM(((q_max + 1) * SUB, LANE), F32),
        pltpu.VMEM((2 * ep * rows_blk + SUB, LANE), F32),
    )

    ag.drain()


def solution(mesh):
    ep = mesh.shape["ep"]

    def device_step(tokens, expert_ids, norm_gain, w_router, w_gate, w_up, w_down):
        tok, top_k = expert_ids.shape
        width = tokens.shape[1]
        e_local, _, ff = w_gate.shape
        pairs = tok * top_k
        send_max = 2 * pairs // ep
        recv_max = 3 * pairs // 2
        tiles = (recv_max + e_local * (TILE - 1)) // TILE
        half_w = width // 2
        fcol = 256
        chips = ep // 2
        rows_blk = tok * SUB
        vm = pl.BlockSpec(memory_space=pltpu.VMEM)
        hbm = pl.BlockSpec(memory_space=pl.ANY)
        sm = pl.BlockSpec(memory_space=pltpu.SMEM)
        dma = pltpu.SemaphoreType.DMA
        i32 = jnp.int32
        groups = (ep, send_max)
        u0, u1, slot, src, first, last, te, gate = pl.pallas_call(
            functools.partial(plan_kernel, ep, tiles),
            out_shape=[
                jax.ShapeDtypeStruct((ep * tok, half_w), BF16),
                jax.ShapeDtypeStruct((tok, half_w), BF16),
                jax.ShapeDtypeStruct((e_local, SUB, ep * tok), F32),
                jax.ShapeDtypeStruct(groups, i32),
                jax.ShapeDtypeStruct(groups, i32),
                jax.ShapeDtypeStruct((ep, tok), i32),
                jax.ShapeDtypeStruct((1, LANE), i32),
                jax.ShapeDtypeStruct(groups, F32),
            ],
            in_specs=[vm] * 4,
            out_specs=[vm] * 8,
            scratch_shapes=[
                pltpu.VMEM((w_router.shape[1], tok), F32),
                pltpu.VMEM((ep, top_k, tok), i32),
                pltpu.VMEM((ep, e_local, tok), F32),
                dma((2, ep)),
                dma((2, ep)),
                dma((14,)),
                dma((14,)),
            ],
            compiler_params=pltpu.CompilerParams(collective_id=0, has_side_effects=True),
            name="moe_plan",
        )(tokens, expert_ids.T, norm_gain[None, :], w_router)
        return pl.pallas_call(
            functools.partial(moe_kernel, ep, tiles),
            out_shape=jax.ShapeDtypeStruct((tok, width), BF16),
            in_specs=[sm] * 5 + [hbm, vm, vm, hbm, hbm, hbm, hbm],
            out_specs=vm,
            scratch_shapes=[
                pltpu.VMEM((2, ep * tok, half_w), BF16),
                pltpu.VMEM((tok, width), BF16),
                pltpu.VMEM((tiles * TILE, ff), BF16),
                *[pltpu.VMEM((e_local, half_w, fcol), BF16)] * 4,
                pltpu.VMEM((2 * chips * rows_blk, LANE), F32),
                pltpu.VMEM((2 * rows_blk, LANE), F32),
                pltpu.VMEM((4 * rows_blk + SUB, LANE), F32),
                dma((2,)),
                dma((4,)),
                dma((14,)),
                dma((14,)),
                dma((2, chips)),
                dma((2, chips)),
                dma((2, 2)),
                dma((2, 2)),
                dma((2, 4)),
                dma((2, 4)),
            ],
            compiler_params=pltpu.CompilerParams(
                collective_id=1, has_side_effects=True, vmem_limit_bytes=67_043_328),
            name="moe_block",
        )(te, src, first, last, gate, u0, u1, slot, tokens, w_gate, w_up, w_down)

    row_spec = P(("dp", "ep"), None)
    expert_spec = P("ep", None, None)
    return jax.shard_map(
        device_step, mesh=mesh,
        in_specs=(row_spec, row_spec, P(None), P(None, None), expert_spec, expert_spec, expert_spec),
        out_specs=row_spec, check_vma=False)
```

```python
import functools

import jax
import jax.numpy as jnp
from jax import lax
from jax.experimental import pallas as pl
from jax.experimental.pallas import tpu as pltpu
from jax.sharding import PartitionSpec as P

NORM_EPS = 1e-5
TILE = 128
SUB = 8
LANE = 128
F32 = jnp.float32
BF16 = jnp.bfloat16
MESH = pl.DeviceIdType.MESH


def dot(a, b, dims=(((1,), (0,)), ((), ()))):
    return lax.dot_general(a, b, dims, preferred_element_type=F32)


NT_DIMS = (((1,), (1,)), ((), ()))


class Place:
    def __init__(self, ep):
        self.ep = ep
        self.me = lax.axis_index("ep")
        self.xi, self.core = self.me // 2, self.me % 2
        self.chips = ep // 2
        self.right, self.left, self.far = self.dev(1, self.core), self.dev(-1, self.core), self.dev(2, self.core)
        self.partner = self.dev(0, 1 - self.core)

    def dev(self, dx, c):
        return lax.rem(self.xi + dx + self.chips, self.chips) * 2 + c

    def signal_all(self):
        barrier = pltpu.get_barrier_semaphore()
        for d in range(1, self.ep):
            pl.semaphore_signal(barrier, inc=1, device_id={"ep": lax.rem(self.me + d, self.ep)}, device_id_type=MESH)
        return barrier


class Gather:
    def __init__(self, pc, ref, send, recv, tok, own=None):
        self.pc, self.ref, self.send, self.recv, self.tok, self.own = pc, ref, send, recv, tok, own

    def copy(self, j, block, r, target, own=False):
        hr = self.tok // 2
        rows = pl.ds(pl.multiple_of(block * self.tok + r * hr, hr), hr)
        dst = self.ref.at[rows, :]
        src = self.own.at[pl.ds(r * hr, hr), :] if own and self.own is not None else dst
        return pltpu.make_async_remote_copy(
            src, dst, self.send.at[j], self.recv.at[j], device_id={"ep": target}, device_id_type=MESH)

    def start(self):
        p = self.pc
        self.copy(0, p.me, 0, p.right, True).start()
        self.copy(2, p.me, 1, p.left, True).start()
        self.copy(1, p.me, 1, p.right, True).start()
        self.copy(3, p.me, 0, p.left, True).start()
        self.copy(6, p.me, 0, p.partner, True).start()
        self.copy(7, p.me, 1, p.partner, True).start()

    def forward(self):
        p = self.pc
        self.copy(0, p.left, 0, p.right).wait_recv()
        self.copy(4, p.left, 0, p.right).start()
        self.copy(8, p.left, 0, p.partner).start()
        self.copy(2, p.right, 1, p.left).wait_recv()
        self.copy(5, p.right, 1, p.left).start()
        self.copy(11, p.right, 1, p.partner).start()

    def rest(self):
        p = self.pc
        self.copy(1, p.left, 1, p.right).wait_recv()
        self.copy(9, p.left, 1, p.partner).start()
        self.copy(3, p.right, 0, p.left).wait_recv()
        self.copy(10, p.right, 0, p.partner).start()

    def last(self):
        p = self.pc
        self.copy(4, p.far, 0, p.right).wait_recv()
        self.copy(12, p.far, 0, p.partner).start()
        self.copy(5, p.far, 1, p.left).wait_recv()
        self.copy(13, p.far, 1, p.partner).start()

    def finish(self):
        p = self.pc
        for j, (dx, r) in enumerate(((0, 0), (0, 1), (-1, 0), (-1, 1), (1, 0), (1, 1), (2, 0), (2, 1))):
            self.copy(6 + j, p.dev(dx, 1 - p.core), r, p.partner).wait_recv()

    def drain(self):
        for j in range(14):
            self.copy(j, self.pc.me, 0, self.pc.right).wait_send()


def plan_kernel(
    ep, tiles,
    x_ref, ids_ref, gain_ref, wr_ref,
    u0_ref, u1_ref, slot_ref, src_v, first_v, last_v, te_v, gate_v,
    p_ref, id_land, p_land,
    small_send, small_recv, ag_send, ag_recv,
):
    pc = Place(ep)
    me = pc.me
    tok, width = x_ref.shape
    half_w = width // 2
    e_local = slot_ref.shape[0]
    q_max = src_v.shape[1]
    barrier = pc.signal_all()

    x32 = x_ref[...].astype(F32)
    inv = lax.rsqrt(jnp.mean(x32 * x32, axis=1, keepdims=True) + NORM_EPS)
    u_own = (x32 * inv * gain_ref[...].astype(F32)[None, :]).astype(BF16)
    own_rows = pl.ds(pl.multiple_of(me * tok, tok), tok)
    u0_ref[own_rows, :] = u_own[:, :half_w]
    u1_ref[...] = u_own[:, half_w:]

    pl.semaphore_wait(barrier, ep - 1)

    ag = Gather(pc, u0_ref, ag_send, ag_recv, tok)
    ag.start()

    logits = dot(wr_ref[...], u_own, NT_DIMS)
    ex = jnp.exp(logits - jnp.max(logits, axis=0, keepdims=True))
    p_ref[...] = ex / jnp.sum(ex, axis=0, keepdims=True)
    id_land[me] = ids_ref[...]
    p_land[me] = p_ref[pl.ds(pl.multiple_of(me * e_local, e_local), e_local), :]

    def small(d, kind, target):
        if kind == 0:
            src, dst = ids_ref, id_land.at[me]
        else:
            src, dst = p_ref.at[pl.ds(pl.multiple_of(target * e_local, e_local), e_local), :], p_land.at[me]
        return pltpu.make_async_remote_copy(
            src, dst, small_send.at[kind, d], small_recv.at[kind, d], device_id={"ep": target}, device_id_type=MESH)

    for kind in range(2):
        for d in range(1, ep):
            small(d, kind, lax.rem(me + d, ep)).start()
    for kind in range(2):
        for d in range(1, ep):
            small(d, kind, lax.rem(me + d, ep)).wait_recv()

    base = me * e_local
    sub_i = lax.broadcasted_iota(jnp.int32, (e_local, LANE), 0)
    lane_i = lax.broadcasted_iota(jnp.int32, (e_local, LANE), 1)
    tri = (lax.broadcasted_iota(jnp.int32, (LANE, LANE), 0) < lax.broadcasted_iota(jnp.int32, (LANE, LANE), 1)).astype(BF16)
    member = []
    for b in range(ep):
        ids_b = id_land[b]
        m = jnp.zeros((e_local, LANE), F32)
        for k in range(ids_b.shape[0]):
            m = m + jnp.where(ids_b[k:k + 1, :] == base + sub_i, 1.0, 0.0)
        member.append(m)
    stack = jnp.concatenate(member, axis=0)
    before = dot(stack.astype(BF16), tri)
    total = jnp.sum(stack, axis=1, keepdims=True)
    run = jnp.zeros((e_local, 1), F32)
    pos = []
    for b in range(ep):
        pos.append(before[b * e_local:(b + 1) * e_local] + run)
        run = run + total[b * e_local:(b + 1) * e_local]
    tiles_e = jnp.floor((run + (TILE - 1)) * (1.0 / TILE))
    start = jnp.zeros((e_local, 1), F32)
    sub_c = lax.broadcasted_iota(jnp.int32, (e_local, 1), 0)
    for e in range(e_local):
        start = start + jnp.where(sub_c > e, tiles_e[e:e + 1, :], 0.0)
    tile_end = start + tiles_e
    te = jnp.sum(jnp.where(tile_end <= lane_i.astype(F32), 1.0, 0.0), axis=0, keepdims=True)
    te_v[...] = jnp.clip(te.astype(jnp.int32), 0, e_local - 1)
    count = jnp.concatenate([jnp.sum(m, axis=0, keepdims=True) for m in member], axis=0)
    first_rank = dot(count.astype(BF16), tri)
    last_row = jnp.where(count > 0, first_rank + count - 1.0, q_max * 1.0)
    last_v[...] = jnp.clip(last_row.astype(jnp.int32), 0, q_max)
    q_row = lax.broadcasted_iota(jnp.int32, (q_max, LANE), 0).astype(F32)
    q_lane = lax.broadcasted_iota(jnp.int32, (e_local, q_max), 1).astype(F32)
    for b in range(ep):
        m = member[b]
        slot = jnp.where(m > 0, start * TILE + pos[b], -1.0)
        slot_ref[:, :, b * LANE:(b + 1) * LANE] = jnp.broadcast_to(slot[:, None, :], (e_local, SUB, LANE))
        pre = jnp.zeros((e_local, LANE), F32)
        for e in range(e_local):
            pre = pre + jnp.where(sub_i > e, m[e:e + 1, :], 0.0)
        fr, ct = first_rank[b:b + 1], count[b:b + 1]
        rank = jnp.where(m > 0, fr + pre, 300.0)
        hi = jnp.floor(slot * (1.0 / 64))
        pb = p_land[b]
        g1 = pb.astype(BF16).astype(F32)
        g2 = (pb - g1).astype(BF16).astype(F32)
        g3 = pb - g1 - g2
        feats = jnp.concatenate([rank, hi, slot - hi * 64.0, jnp.broadcast_to(fr, m.shape), g1, g2, g3, pre], axis=0)
        hot = jnp.where((q_row >= fr) & (q_row < fr + ct), 1.0, 0.0).astype(BF16)
        got = dot(feats.astype(BF16), hot, NT_DIMS)
        e8 = e_local
        sel = got[0:e8] == q_lane
        src = jnp.sum(jnp.where(sel, got[e8:2 * e8] * 64.0 + got[2 * e8:3 * e8], 0.0), axis=0, keepdims=True)
        gate = jnp.sum(jnp.where(sel, got[4 * e8:5 * e8] + got[5 * e8:6 * e8] + got[6 * e8:7 * e8], 0.0), axis=0, keepdims=True)
        src_v[b:b + 1, :] = jnp.clip(src.astype(jnp.int32), 0, tiles * TILE - 1)
        first_v[b:b + 1, :] = (got[3 * e8:3 * e8 + 1] == q_lane[0:1]).astype(jnp.int32)
        gate_v[b:b + 1, :] = gate

    ag.forward()
    ag.rest()
    ag.last()
    ag.finish()
    ag.drain()
    for kind in range(2):
        for d in range(1, ep):
            small(d, kind, lax.rem(me + d, ep)).wait_send()


def up_kernel(
    ep, tiles,
    te_s, u0_hbm, u1_ref, slot_ref, w1_hbm, w3_hbm,
    h_ref,
    u_all, ring0, ring1, ring2, ring3,
    in_sem, ring_sem, ag_send, ag_recv,
):
    pc = Place(ep)
    me, core, chips, dev = pc.me, pc.core, pc.chips, pc.dev
    right, left, partner, far = pc.right, pc.left, pc.partner, pc.far
    ring = (ring0, ring1, ring2, ring3)
    tok, half_w = u1_ref.shape
    ff = h_ref.shape[1]
    e_local, _, fcol = ring0.shape
    n_fs = ff // fcol

    def w13_copy(m, buf):
        kk, ffi = m // (2 * n_fs), (m % (2 * n_fs)) // 2
        rows = pl.ds(pl.multiple_of(kk * half_w, half_w), half_w)
        cols = pl.ds(pl.multiple_of(ffi * fcol, fcol), fcol)
        return [pltpu.make_async_copy(w.at[:, rows, cols], ring[buf], ring_sem.at[buf]) for w in (w1_hbm, w3_hbm)]

    for m in range(4):
        w13_copy(m, m)[m % 2].start()

    barrier = pc.signal_all()

    pltpu.make_async_copy(u0_hbm, u_all.at[0], in_sem).start()
    own_rows = pl.ds(pl.multiple_of(me * tok, tok), tok)
    pl.semaphore_wait(barrier, ep - 1)
    ag = Gather(pc, u_all.at[1], ag_send, ag_recv, tok, own=u1_ref)
    ag.start()
    u_all[1, own_rows, :] = u1_ref[...]
    pltpu.make_async_copy(u0_hbm, u_all.at[0], in_sem).wait()

    def tile_expert(i):
        return te_s[0, i]

    def phase_one(ug, acc):
        t_iota = lax.broadcasted_iota(jnp.int32, (TILE, ep * tok), 0).astype(F32)

        def gather(k, lo, hi, un):
            def body(g, carry):
                for j in range(un):
                    i = lo + g * un + j
                    row = slot_ref[tile_expert(i)][0:1] - lax.convert_element_type(i * TILE, F32)
                    hot = jnp.where(row == t_iota, 1.0, 0.0).astype(BF16)
                    ug[pl.ds(pl.multiple_of(i * TILE, TILE), TILE), :] = dot(hot, u_all[k]).astype(BF16)
                return carry

            lax.fori_loop(0, (hi - lo) // un, body, 0)

        def units(k):
            def two_units(fp, carry):
                for b1 in (0, 2):
                    fs = 2 * fp + b1 // 2
                    n = k * 2 * n_fs + 2 * fs
                    for which in range(2):
                        w13_copy(n, b1 + which)[which].wait()
                    for which in range(2):
                        for i in range(tiles):
                            rows = pl.ds(i * TILE, TILE)
                            d = dot(ug[rows, :], ring[b1 + which][tile_expert(i)])
                            if k == 0:
                                acc[which, fs, rows, :] = d
                            elif which == 0:
                                acc[0, fs, rows, :] = acc[0, fs, rows, :] + d
                            else:
                                g = acc[0, fs, rows, :]
                                hcols = pl.ds(pl.multiple_of(fs * fcol, fcol), fcol)
                                h_ref[rows, hcols] = (g / (1.0 + jnp.exp(-g)) * (acc[1, fs, rows, :] + d)).astype(BF16)
                        if k == 0:
                            w13_copy(n + 4 + which, b1 + which)[which].start()
                        else:
                            @pl.when(fp == 0)
                            def _():
                                w13_copy(n + 4 + which, b1 + which)[which].start()
                return carry

            lax.fori_loop(0, n_fs // 2, two_units, 0)

        mid = tiles // 2
        gather(0, 0, mid, 3)
        ag.forward()
        gather(0, mid, tiles, 5)
        ag.rest()
        units(0)
        ag.last()
        ag.finish()
        gather(1, 0, mid, 3)
        gather(1, mid, tiles, 5)
        units(1)

    pl.run_scoped(
        phase_one,
        pltpu.VMEM((tiles * TILE, half_w), BF16),
        pltpu.VMEM((2, n_fs, tiles * TILE, fcol), F32),
    )
    ag.drain()


def down_kernel(
    ep, tiles,
    te_s, src_s, first_s, last_s, gate_s,
    h_hbm, x_ref, w2_hbm,
    out_ref,
    h_ref, ring0, ring1, ring2, ring3,
    recv_a, recv_h, recv_d,
    in_sem, ring_sem,
    a_send, a_recv, h_send, h_recv, d_send, d_recv,
):
    pc = Place(ep)
    me, core, chips, dev = pc.me, pc.core, pc.chips, pc.dev
    right, left, partner, far = pc.right, pc.left, pc.partner, pc.far
    ring = (ring0, ring1, ring2, ring3)
    tok, width = x_ref.shape
    q_max = src_s.shape[1]
    half_w = width // 2
    fcol = ring0.shape[2]
    rows_blk = tok * SUB

    def tile_expert(i):
        return te_s[0, i]

    def w2_copy(cs, buf):
        cols = pl.ds(pl.multiple_of(cs * fcol, fcol), fcol)
        return pltpu.make_async_copy(w2_hbm.at[:, :, cols], ring[buf], ring_sem.at[buf])

    h_in = pltpu.make_async_copy(h_hbm, h_ref, in_sem)
    h_in.start()
    for b in range(4):
        w2_copy(b, b).start()
    barrier = pc.signal_all()
    pl.semaphore_wait(barrier, ep - 1)
    h_in.wait()

    def phase_two(o3, pbuf, accb):
        n_slice = half_w // fcol
        order = (2, 1, 3, 0)
        o_rows = o3.reshape(o3.shape[0] // SUB, SUB, LANE)
        p_rows = pbuf.reshape(pbuf.shape[0] // SUB, SUB, LANE)
        pbuf[q_max * SUB:(q_max + 1) * SUB, :] = jnp.zeros((SUB, LANE), F32)

        def block(q, s):
            return pl.ds(pl.multiple_of((q * ep + s) * rows_blk, rows_blk), rows_blk)

        def combine(q, s):
            un = 8

            def pairs(i, run):
                for j in range(un):
                    qq = i * un + j
                    row = o_rows[src_s[s, qq]]
                    run = jnp.where(jnp.full((SUB, LANE), first_s[s, qq], jnp.int32) == 1, 0.0, run) + gate_s[s, qq] * row
                    pbuf[pl.ds(pl.multiple_of(qq * SUB, SUB), SUB), :] = run
                return run

            lax.fori_loop(0, q_max // un, pairs, jnp.zeros((SUB, LANE), F32))

            def tokens(i, carry):
                for j in range(un):
                    t = i * un + j
                    dst = pl.ds(pl.multiple_of((q * ep + s) * rows_blk + t * SUB, SUB), SUB)
                    accb[dst, :] = p_rows[last_s[s, t]]
                return carry

            lax.fori_loop(0, tok // un, tokens, 0)

        def a_copy(q, j):
            rows = pl.ds((q * chips + j) * rows_blk, rows_blk)
            return pltpu.make_async_remote_copy(
                accb.at[block(q, dev(order[j], 1 - core)), :], recv_a.at[rows, :], a_send.at[q, j], a_recv.at[q, j],
                device_id={"ep": partner}, device_id_type=MESH)

        def a_add(q, j):
            a_copy(q, j).wait_recv()
            mine = block(q, dev(order[j], core))
            accb[mine, :] = accb[mine, :] + recv_a[(q * chips + j) * rows_blk:(q * chips + j + 1) * rows_blk, :]

        hb = rows_blk // 2

        def half(q, s, r):
            return pl.ds(pl.multiple_of((q * ep + s) * rows_blk + r * hb, hb), hb)

        def h_copy(q, side):
            return pltpu.make_async_remote_copy(
                accb.at[half(q, far, side), :], recv_h.at[pl.ds((q * 2 + side) * hb, hb), :], h_send.at[q, side], h_recv.at[q, side],
                device_id={"ep": left if side else right}, device_id_type=MESH)

        def d_copy(q, side, r):
            s = left if side else right
            return pltpu.make_async_remote_copy(
                accb.at[half(q, s, r), :], recv_d.at[pl.ds((q * 2 + side) * rows_blk + r * hb, hb), :],
                d_send.at[q, side * 2 + r], d_recv.at[q, side * 2 + r], device_id={"ep": s}, device_id_type=MESH)

        def relay(q):
            for side in range(2):
                h_copy(q, side).wait_recv()
                s = left if side else right
                mine = half(q, s, side)
                accb[mine, :] = accb[mine, :] + recv_h[(q * 2 + side) * hb:(q * 2 + side + 1) * hb, :]
                d_copy(q, side, side).start()

        def down(q):
            def body(jp, carry):
                for b1 in range(4):
                    j = jp * 4 + b1
                    if q == 1 and b1 == 1:
                        relay(0)
                    w2_copy(q * n_slice + j, b1).wait()
                    for i in range(tiles):
                        o = dot(h_ref[i * TILE:(i + 1) * TILE, :], ring[b1][tile_expert(i)]).astype(BF16).astype(F32)
                        for v in range(fcol // LANE):
                            o3[pl.ds(i * TILE * SUB + j * (fcol // LANE) + v, TILE, stride=SUB), :] = o[:, v * LANE:(v + 1) * LANE]
                    if q == 0:
                        w2_copy(n_slice + j, b1).start()
                return carry

            body(0, 0)

        def scatter(q):
            for j in range(chips):
                combine(q, dev(order[j], 1 - core))
                a_copy(q, j).start()
                combine(q, dev(order[j], core))
                a_add(q, j)
                if j == 0:
                    h_copy(q, 0).start()
                    h_copy(q, 1).start()
                elif j == 1:
                    d_copy(q, 0, 1).start()
                elif j == 2:
                    d_copy(q, 1, 0).start()

        def finish(q):
            for side in range(2):
                for r in range(2):
                    d_copy(q, side, r).wait_recv()
            for v in range(half_w // LANE):
                cols = slice(q * half_w + v * LANE, q * half_w + (v + 1) * LANE)
                own = accb[pl.ds((q * ep + me) * rows_blk + v, tok, stride=SUB), :]
                d0 = recv_d[pl.ds(q * 2 * rows_blk + v, tok, stride=SUB), :]
                d1 = recv_d[pl.ds((q * 2 + 1) * rows_blk + v, tok, stride=SUB), :]
                out_ref[:, cols] = (x_ref[:, cols].astype(F32) + (own + d0 + d1)).astype(BF16)

        down(0)
        scatter(0)
        down(1)
        scatter(1)
        relay(1)
        finish(0)
        finish(1)
        for q in range(2):
            for j in range(chips):
                a_copy(q, j).wait_send()
            for side in range(2):
                h_copy(q, side).wait_send()
                for r in range(2):
                    d_copy(q, side, r).wait_send()

    pl.run_scoped(
        phase_two,
        pltpu.VMEM((tiles * TILE * SUB + SUB, LANE), F32),
        pltpu.VMEM(((q_max + 1) * SUB, LANE), F32),
        pltpu.VMEM((2 * ep * rows_blk + SUB, LANE), F32),
    )


def solution(mesh):
    ep = mesh.shape["ep"]

    def device_step(tokens, expert_ids, norm_gain, w_router, w_gate, w_up, w_down):
        tok, top_k = expert_ids.shape
        width = tokens.shape[1]
        e_local, _, ff = w_gate.shape
        pairs = tok * top_k
        send_max = 2 * pairs // ep
        recv_max = 3 * pairs // 2
        tiles = (recv_max + e_local * (TILE - 1)) // TILE
        half_w = width // 2
        fcol = 256
        chips = ep // 2
        rows_blk = tok * SUB
        vm = pl.BlockSpec(memory_space=pltpu.VMEM)
        hbm = pl.BlockSpec(memory_space=pl.ANY)
        sm = pl.BlockSpec(memory_space=pltpu.SMEM)
        dma = pltpu.SemaphoreType.DMA
        i32 = jnp.int32
        groups = (ep, send_max)
        u0, u1, slot, src, first, last, te, gate = pl.pallas_call(
            functools.partial(plan_kernel, ep, tiles),
            out_shape=[
                jax.ShapeDtypeStruct((ep * tok, half_w), BF16),
                jax.ShapeDtypeStruct((tok, half_w), BF16),
                jax.ShapeDtypeStruct((e_local, SUB, ep * tok), F32),
                jax.ShapeDtypeStruct(groups, i32),
                jax.ShapeDtypeStruct(groups, i32),
                jax.ShapeDtypeStruct((ep, tok), i32),
                jax.ShapeDtypeStruct((1, LANE), i32),
                jax.ShapeDtypeStruct(groups, F32),
            ],
            in_specs=[vm] * 4,
            out_specs=[vm] * 8,
            scratch_shapes=[
                pltpu.VMEM((w_router.shape[1], tok), F32),
                pltpu.VMEM((ep, top_k, tok), i32),
                pltpu.VMEM((ep, e_local, tok), F32),
                dma((2, ep)),
                dma((2, ep)),
                dma((14,)),
                dma((14,)),
            ],
            compiler_params=pltpu.CompilerParams(collective_id=0, has_side_effects=True),
            name="moe_plan",
        )(tokens, expert_ids.T, norm_gain, w_router.T)
        ring = [pltpu.VMEM((e_local, half_w, fcol), BF16)] * 4
        h = pl.pallas_call(
            functools.partial(up_kernel, ep, tiles),
            out_shape=jax.ShapeDtypeStruct((tiles * TILE, ff), BF16),
            in_specs=[sm, hbm, vm, vm, hbm, hbm],
            out_specs=vm,
            scratch_shapes=[
                pltpu.VMEM((2, ep * tok, half_w), BF16),
                *ring,
                dma(()),
                dma((4,)),
                dma((14,)),
                dma((14,)),
            ],
            compiler_params=pltpu.CompilerParams(
                collective_id=1, has_side_effects=True, vmem_limit_bytes=67_043_328),
            name="moe_up",
        )(te, u0, u1, slot, w_gate, w_up)
        return pl.pallas_call(
            functools.partial(down_kernel, ep, tiles),
            out_shape=jax.ShapeDtypeStruct((tok, width), BF16),
            in_specs=[sm] * 5 + [hbm, vm, hbm],
            out_specs=vm,
            scratch_shapes=[
                pltpu.VMEM((tiles * TILE, ff), BF16),
                *ring,
                pltpu.VMEM((2 * chips * rows_blk, LANE), F32),
                pltpu.VMEM((2 * rows_blk, LANE), F32),
                pltpu.VMEM((4 * rows_blk + SUB, LANE), F32),
                dma(()),
                dma((4,)),
                dma((2, chips)),
                dma((2, chips)),
                dma((2, 2)),
                dma((2, 2)),
                dma((2, 4)),
                dma((2, 4)),
            ],
            compiler_params=pltpu.CompilerParams(
                collective_id=2, has_side_effects=True, vmem_limit_bytes=67_043_328),
            name="moe_down",
        )(te, src, first, last, gate, h, tokens, w_down)

    row_spec = P(("dp", "ep"), None)
    expert_spec = P("ep", None, None)
    return jax.shard_map(
        device_step, mesh=mesh,
        in_specs=(row_spec, row_spec, P(None), P(None, None), expert_spec, expert_spec, expert_spec),
        out_specs=row_spec, check_vma=False)
```

```python
import functools

import jax
import jax.numpy as jnp
from jax import lax
from jax.experimental import pallas as pl
from jax.experimental.pallas import tpu as pltpu
from jax.sharding import PartitionSpec as P

NORM_EPS = 1e-5
TILE = 128
SUB = 8
LANE = 128
F32 = jnp.float32
BF16 = jnp.bfloat16
MESH = pl.DeviceIdType.MESH


def dot(a, b, dims=(((1,), (0,)), ((), ()))):
    return lax.dot_general(a, b, dims, preferred_element_type=F32)


NT_DIMS = (((1,), (1,)), ((), ()))


class Place:
    def __init__(self, ep):
        self.ep = ep
        self.me = lax.axis_index("ep")
        self.xi, self.core = self.me // 2, self.me % 2
        self.chips = ep // 2
        self.right, self.left, self.far = self.dev(1, self.core), self.dev(-1, self.core), self.dev(2, self.core)
        self.partner = self.dev(0, 1 - self.core)

    def dev(self, dx, c):
        return lax.rem(self.xi + dx + self.chips, self.chips) * 2 + c

    def signal_all(self):
        barrier = pltpu.get_barrier_semaphore()
        for d in range(1, self.ep):
            pl.semaphore_signal(barrier, inc=1, device_id={"ep": lax.rem(self.me + d, self.ep)}, device_id_type=MESH)
        return barrier


class Gather:
    def __init__(self, pc, ref, send, recv, tok, own=None):
        self.pc, self.ref, self.send, self.recv, self.tok, self.own = pc, ref, send, recv, tok, own

    def copy(self, j, block, r, target, own=False):
        hr = self.tok // 2
        rows = pl.ds(pl.multiple_of(block * self.tok + r * hr, hr), hr)
        dst = self.ref.at[rows, :]
        src = self.own.at[pl.ds(r * hr, hr), :] if own and self.own is not None else dst
        return pltpu.make_async_remote_copy(
            src, dst, self.send.at[j], self.recv.at[j], device_id={"ep": target}, device_id_type=MESH)

    def start(self):
        p = self.pc
        self.copy(0, p.me, 0, p.right, True).start()
        self.copy(2, p.me, 1, p.left, True).start()
        self.copy(1, p.me, 1, p.right, True).start()
        self.copy(3, p.me, 0, p.left, True).start()
        self.copy(6, p.me, 0, p.partner, True).start()
        self.copy(7, p.me, 1, p.partner, True).start()

    def forward(self):
        p = self.pc
        self.copy(0, p.left, 0, p.right).wait_recv()
        self.copy(4, p.left, 0, p.right).start()
        self.copy(8, p.left, 0, p.partner).start()
        self.copy(2, p.right, 1, p.left).wait_recv()
        self.copy(5, p.right, 1, p.left).start()
        self.copy(11, p.right, 1, p.partner).start()

    def rest(self):
        p = self.pc
        self.copy(1, p.left, 1, p.right).wait_recv()
        self.copy(9, p.left, 1, p.partner).start()
        self.copy(3, p.right, 0, p.left).wait_recv()
        self.copy(10, p.right, 0, p.partner).start()

    def last(self):
        p = self.pc
        self.copy(4, p.far, 0, p.right).wait_recv()
        self.copy(12, p.far, 0, p.partner).start()
        self.copy(5, p.far, 1, p.left).wait_recv()
        self.copy(13, p.far, 1, p.partner).start()

    def finish(self):
        p = self.pc
        for j, (dx, r) in enumerate(((0, 0), (0, 1), (-1, 0), (-1, 1), (1, 0), (1, 1), (2, 0), (2, 1))):
            self.copy(6 + j, p.dev(dx, 1 - p.core), r, p.partner).wait_recv()

    def drain(self):
        for j in range(14):
            self.copy(j, self.pc.me, 0, self.pc.right).wait_send()


def plan_kernel(
    ep, tiles,
    x_ref, ids_ref, gain_ref, wr_ref,
    u0_ref, u1_ref, slot_ref, src_v, first_v, last_v, te_v, gate_v,
    p_ref, id_land, p_land,
    small_send, small_recv, ag_send, ag_recv,
):
    pc = Place(ep)
    me = pc.me
    tok, width = x_ref.shape
    part_w = u0_ref.shape[1]
    e_local = slot_ref.shape[0]
    q_max = src_v.shape[1]
    barrier = pc.signal_all()

    x32 = x_ref[...].astype(F32)
    inv = lax.rsqrt(jnp.mean(x32 * x32, axis=1, keepdims=True) + NORM_EPS)
    u_own = (x32 * inv * gain_ref[...].astype(F32)[None, :]).astype(BF16)
    own_rows = pl.ds(pl.multiple_of(me * tok, tok), tok)
    u0_ref[own_rows, :] = u_own[:, :part_w]
    for k in range(1, width // part_w):
        u1_ref[k - 1] = u_own[:, k * part_w:(k + 1) * part_w]

    pl.semaphore_wait(barrier, ep - 1)

    ag = Gather(pc, u0_ref, ag_send, ag_recv, tok)
    ag.start()

    logits = dot(wr_ref[...], u_own, NT_DIMS)
    ex = jnp.exp(logits - jnp.max(logits, axis=0, keepdims=True))
    p_ref[...] = ex / jnp.sum(ex, axis=0, keepdims=True)
    id_land[me] = ids_ref[...]
    p_land[me] = p_ref[pl.ds(pl.multiple_of(me * e_local, e_local), e_local), :]

    def small(d, kind, target):
        if kind == 0:
            src, dst = ids_ref, id_land.at[me]
        else:
            src, dst = p_ref.at[pl.ds(pl.multiple_of(target * e_local, e_local), e_local), :], p_land.at[me]
        return pltpu.make_async_remote_copy(
            src, dst, small_send.at[kind, d], small_recv.at[kind, d], device_id={"ep": target}, device_id_type=MESH)

    for kind in range(2):
        for d in range(1, ep):
            small(d, kind, lax.rem(me + d, ep)).start()
    for kind in range(2):
        for d in range(1, ep):
            small(d, kind, lax.rem(me + d, ep)).wait_recv()

    base = me * e_local
    sub_i = lax.broadcasted_iota(jnp.int32, (e_local, LANE), 0)
    lane_i = lax.broadcasted_iota(jnp.int32, (e_local, LANE), 1)
    tri = (lax.broadcasted_iota(jnp.int32, (LANE, LANE), 0) < lax.broadcasted_iota(jnp.int32, (LANE, LANE), 1)).astype(BF16)
    member = []
    for b in range(ep):
        ids_b = id_land[b]
        m = jnp.zeros((e_local, LANE), F32)
        for k in range(ids_b.shape[0]):
            m = m + jnp.where(ids_b[k:k + 1, :] == base + sub_i, 1.0, 0.0)
        member.append(m)
    stack = jnp.concatenate(member, axis=0)
    before = dot(stack.astype(BF16), tri)
    total = jnp.sum(stack, axis=1, keepdims=True)
    run = jnp.zeros((e_local, 1), F32)
    pos = []
    for b in range(ep):
        pos.append(before[b * e_local:(b + 1) * e_local] + run)
        run = run + total[b * e_local:(b + 1) * e_local]
    tiles_e = jnp.floor((run + (TILE - 1)) * (1.0 / TILE))
    start = jnp.zeros((e_local, 1), F32)
    sub_c = lax.broadcasted_iota(jnp.int32, (e_local, 1), 0)
    for e in range(e_local):
        start = start + jnp.where(sub_c > e, tiles_e[e:e + 1, :], 0.0)
    tile_end = start + tiles_e
    te = jnp.sum(jnp.where(tile_end <= lane_i.astype(F32), 1.0, 0.0), axis=0, keepdims=True)
    te_v[...] = jnp.clip(te.astype(jnp.int32), 0, e_local - 1)
    count = jnp.concatenate([jnp.sum(m, axis=0, keepdims=True) for m in member], axis=0)
    first_rank = dot(count.astype(BF16), tri)
    last_row = jnp.where(count > 0, first_rank + count - 1.0, q_max * 1.0)
    last_v[...] = jnp.clip(last_row.astype(jnp.int32), 0, q_max)
    q_row = lax.broadcasted_iota(jnp.int32, (q_max, LANE), 0).astype(F32)
    q_lane = lax.broadcasted_iota(jnp.int32, (e_local, q_max), 1).astype(F32)
    for b in range(ep):
        m = member[b]
        slot = jnp.where(m > 0, start * TILE + pos[b], -1.0)
        slot_ref[:, :, b * LANE:(b + 1) * LANE] = jnp.broadcast_to(slot[:, None, :], (e_local, SUB, LANE))
        pre = jnp.zeros((e_local, LANE), F32)
        for e in range(e_local):
            pre = pre + jnp.where(sub_i > e, m[e:e + 1, :], 0.0)
        fr, ct = first_rank[b:b + 1], count[b:b + 1]
        rank = jnp.where(m > 0, fr + pre, 300.0)
        hi = jnp.floor(slot * (1.0 / 64))
        pb = p_land[b]
        g1 = pb.astype(BF16).astype(F32)
        g2 = (pb - g1).astype(BF16).astype(F32)
        g3 = pb - g1 - g2
        feats = jnp.concatenate([rank, hi, slot - hi * 64.0, jnp.broadcast_to(fr, m.shape), g1, g2, g3, pre], axis=0)
        hot = jnp.where((q_row >= fr) & (q_row < fr + ct), 1.0, 0.0).astype(BF16)
        got = dot(feats.astype(BF16), hot, NT_DIMS)
        e8 = e_local
        sel = got[0:e8] == q_lane
        src = jnp.sum(jnp.where(sel, got[e8:2 * e8] * 64.0 + got[2 * e8:3 * e8], 0.0), axis=0, keepdims=True)
        gate = jnp.sum(jnp.where(sel, got[4 * e8:5 * e8] + got[5 * e8:6 * e8] + got[6 * e8:7 * e8], 0.0), axis=0, keepdims=True)
        src_v[b:b + 1, :] = jnp.clip(src.astype(jnp.int32), 0, tiles * TILE - 1)
        first_v[b:b + 1, :] = (got[3 * e8:3 * e8 + 1] == q_lane[0:1]).astype(jnp.int32)
        gate_v[b:b + 1, :] = gate

    ag.forward()
    ag.rest()
    ag.last()
    ag.finish()
    ag.drain()
    for kind in range(2):
        for d in range(1, ep):
            small(d, kind, lax.rem(me + d, ep)).wait_send()


def moe_kernel(
    ep, tiles,
    te_s, src_s, first_s, last_s, gate_s,
    u0_hbm, u1_ref, slot_ref, x_hbm, w1_hbm, w3_hbm, w2_hbm,
    out_ref,
    u_all, x_v, h_ref, ring0, ring1, ring2, ring3,
    recv_a, recv_h, recv_d,
    in_sem, ring_sem, ag_send, ag_recv,
    a_send, a_recv, h_send, h_recv, d_send, d_recv,
):
    pc = Place(ep)
    me, core, chips, dev = pc.me, pc.core, pc.chips, pc.dev
    right, left, partner, far = pc.right, pc.left, pc.partner, pc.far
    ring = (ring0, ring1, ring2, ring3)
    tok, width = x_v.shape
    q_max = src_s.shape[1]
    half_w = width // 2
    part_w = ring0.shape[1]
    parts = width // part_w
    rows_blk = tok * SUB

    def up_copy(k, m):
        w = (w1_hbm, w3_hbm)[m % 2]
        rows = pl.ds(pl.multiple_of(k * part_w, part_w), part_w)
        return pltpu.make_async_copy(w.at[:, rows, pl.ds(m // 2 * part_w, part_w)], ring[m], ring_sem.at[m])

    def w2_copy(q, m):
        rows = pl.ds(m % 2 * part_w, part_w)
        return pltpu.make_async_copy(w2_hbm.at[:, rows, pl.ds((2 * q + m // 2) * part_w, part_w)], ring[m], ring_sem.at[m])

    u0_in = pltpu.make_async_copy(u0_hbm, u_all.at[0], in_sem.at[0])
    u0_in.start()
    for m in range(4):
        up_copy(0, m).start()
    x_in = pltpu.make_async_copy(x_hbm, x_v, in_sem.at[1])
    x_in.start()
    barrier = pc.signal_all()
    own_rows = pl.ds(pl.multiple_of(me * tok, tok), tok)
    for k in range(1, parts):
        u_all[k, own_rows, :] = u1_ref[k - 1]
    pl.semaphore_wait(barrier, ep - 1)

    def ag(k):
        return Gather(pc, u_all.at[k], ag_send.at[k], ag_recv.at[k], tok, own=u1_ref.at[k - 1])

    ag(1).start()
    u0_in.wait()

    def tile_expert(i):
        return te_s[0, i]

    def phase_one(ug, acc):
        t_iota = lax.broadcasted_iota(jnp.int32, (TILE, ep * tok), 0).astype(F32)

        def gather(k):
            def tile(i):
                row = slot_ref[tile_expert(i)][0:1] - lax.convert_element_type(i * TILE, F32)
                hot = jnp.where(row == t_iota, 1.0, 0.0).astype(BF16)
                ug[pl.ds(pl.multiple_of(i * TILE, TILE), TILE), :] = dot(hot, u_all[k]).astype(BF16)

            un = 6
            whole = tiles // un

            def body(g, carry):
                for j in range(un):
                    tile(g * un + j)
                return carry

            lax.fori_loop(0, whole, body, 0)
            for i in range(whole * un, tiles):
                tile(jnp.int32(i))

        def slice_dots(k, m, final):
            fs, which = m // 2, m % 2
            up_copy(k, m).wait()
            for i in range(tiles):
                rows = pl.ds(i * TILE, TILE)
                d = dot(ug[rows, :], ring[m][tile_expert(i)])
                if not final:
                    acc[which, fs, rows, :] = jnp.where(k == 0, 0.0, acc[which, fs, rows, :]) + d
                elif which == 0:
                    acc[0, fs, rows, :] = acc[0, fs, rows, :] + d
                else:
                    g = acc[0, fs, rows, :]
                    h_ref[rows, fs * part_w:(fs + 1) * part_w] = (
                        g / (1.0 + jnp.exp(-g)) * (acc[1, fs, rows, :] + d)).astype(BF16)

        def part(k, carry):
            nxt = ag(k + 1)
            gather(k)
            for m in range(4):
                slice_dots(k, m, False)
                up_copy(k + 1, m).start()
                if m == 0:
                    nxt.forward()

                    @pl.when(k < parts - 2)
                    def _():
                        ag(k + 2).start()
                elif m == 1:
                    nxt.rest()
                elif m == 2:
                    nxt.last()
            nxt.finish()
            return carry

        lax.fori_loop(0, parts - 1, part, 0)
        gather(parts - 1)
        for m in range(4):
            slice_dots(parts - 1, m, True)
            w2_copy(0, m).start()

    pl.run_scoped(
        phase_one,
        pltpu.VMEM((tiles * TILE, part_w), BF16),
        pltpu.VMEM((2, 2, tiles * TILE, part_w), F32),
    )

    def phase_two(o3, pbuf, accb):
        order = (2, 1, 3, 0)
        o_rows = o3.reshape(o3.shape[0] // SUB, SUB, LANE)
        p_rows = pbuf.reshape(pbuf.shape[0] // SUB, SUB, LANE)
        pbuf[q_max * SUB:(q_max + 1) * SUB, :] = jnp.zeros((SUB, LANE), F32)

        def block(q, s):
            return pl.ds(pl.multiple_of((q * ep + s) * rows_blk, rows_blk), rows_blk)

        def combine(q, s):
            un = 8

            def pairs(i, run):
                for j in range(un):
                    qq = i * un + j
                    row = o_rows[src_s[s, qq]]
                    run = jnp.where(jnp.full((SUB, LANE), first_s[s, qq], jnp.int32) == 1, 0.0, run) + gate_s[s, qq] * row
                    pbuf[pl.ds(pl.multiple_of(qq * SUB, SUB), SUB), :] = run
                return run

            lax.fori_loop(0, q_max // un, pairs, jnp.zeros((SUB, LANE), F32))

            def tokens(i, carry):
                for j in range(un):
                    t = i * un + j
                    dst = pl.ds(pl.multiple_of((q * ep + s) * rows_blk + t * SUB, SUB), SUB)
                    accb[dst, :] = p_rows[last_s[s, t]]
                return carry

            lax.fori_loop(0, tok // un, tokens, 0)

        def a_copy(q, j):
            rows = pl.ds((q * chips + j) * rows_blk, rows_blk)
            return pltpu.make_async_remote_copy(
                accb.at[block(q, dev(order[j], 1 - core)), :], recv_a.at[rows, :], a_send.at[q, j], a_recv.at[q, j],
                device_id={"ep": partner}, device_id_type=MESH)

        def a_add(q, j):
            a_copy(q, j).wait_recv()
            mine = block(q, dev(order[j], core))
            accb[mine, :] = accb[mine, :] + recv_a[(q * chips + j) * rows_blk:(q * chips + j + 1) * rows_blk, :]

        hb = rows_blk // 2

        def half(q, s, r):
            return pl.ds(pl.multiple_of((q * ep + s) * rows_blk + r * hb, hb), hb)

        def h_copy(q, side):
            return pltpu.make_async_remote_copy(
                accb.at[half(q, far, side), :], recv_h.at[pl.ds((q * 2 + side) * hb, hb), :], h_send.at[q, side], h_recv.at[q, side],
                device_id={"ep": left if side else right}, device_id_type=MESH)

        def d_copy(q, side, r):
            s = left if side else right
            return pltpu.make_async_remote_copy(
                accb.at[half(q, s, r), :], recv_d.at[pl.ds((q * 2 + side) * rows_blk + r * hb, hb), :],
                d_send.at[q, side * 2 + r], d_recv.at[q, side * 2 + r], device_id={"ep": s}, device_id_type=MESH)

        def relay(q):
            for side in range(2):
                h_copy(q, side).wait_recv()
                s = left if side else right
                mine = half(q, s, side)
                accb[mine, :] = accb[mine, :] + recv_h[(q * 2 + side) * hb:(q * 2 + side + 1) * hb, :]
                d_copy(q, side, side).start()

        def down(q):
            lanes = part_w // LANE
            for g in range(2):
                w2_copy(q, 2 * g).wait()
                w2_copy(q, 2 * g + 1).wait()
                for i in range(tiles):
                    rows = slice(i * TILE, (i + 1) * TILE)
                    e = tile_expert(i)
                    o = dot(h_ref[rows, :part_w], ring[2 * g][e]) + dot(h_ref[rows, part_w:], ring[2 * g + 1][e])
                    o = o.astype(BF16).astype(F32)
                    for v in range(lanes):
                        o3[pl.ds(i * TILE * SUB + g * lanes + v, TILE, stride=SUB), :] = o[:, v * LANE:(v + 1) * LANE]
                if q == 0:
                    w2_copy(1, 2 * g).start()
                    w2_copy(1, 2 * g + 1).start()
                elif g == 0:
                    relay(0)

        def scatter(q):
            for j in range(chips):
                combine(q, dev(order[j], 1 - core))
                a_copy(q, j).start()
                combine(q, dev(order[j], core))
                a_add(q, j)
                if j == 0:
                    h_copy(q, 0).start()
                    h_copy(q, 1).start()
                elif j == 1:
                    d_copy(q, 0, 1).start()
                elif j == 2:
                    d_copy(q, 1, 0).start()

        def finish(q):
            for side in range(2):
                for r in range(2):
                    d_copy(q, side, r).wait_recv()
            for v in range(half_w // LANE):
                cols = slice(q * half_w + v * LANE, q * half_w + (v + 1) * LANE)
                own = accb[pl.ds((q * ep + me) * rows_blk + v, tok, stride=SUB), :]
                d0 = recv_d[pl.ds(q * 2 * rows_blk + v, tok, stride=SUB), :]
                d1 = recv_d[pl.ds((q * 2 + 1) * rows_blk + v, tok, stride=SUB), :]
                out_ref[:, cols] = (x_v[:, cols].astype(F32) + (own + d0 + d1)).astype(BF16)

        down(0)
        scatter(0)
        down(1)
        scatter(1)
        relay(1)
        x_in.wait()
        finish(0)
        finish(1)
        for q in range(2):
            for j in range(chips):
                a_copy(q, j).wait_send()
            for side in range(2):
                h_copy(q, side).wait_send()
                for r in range(2):
                    d_copy(q, side, r).wait_send()

    pl.run_scoped(
        phase_two,
        pltpu.VMEM((tiles * TILE * SUB + SUB, LANE), F32),
        pltpu.VMEM(((q_max + 1) * SUB, LANE), F32),
        pltpu.VMEM((2 * ep * rows_blk + SUB, LANE), F32),
    )

    for k in range(1, parts):
        ag(k).drain()


def solution(mesh):
    ep = mesh.shape["ep"]

    def device_step(tokens, expert_ids, norm_gain, w_router, w_gate, w_up, w_down):
        tok, top_k = expert_ids.shape
        width = tokens.shape[1]
        e_local, _, ff = w_gate.shape
        pairs = tok * top_k
        send_max = 2 * pairs // ep
        recv_max = 3 * pairs // 2
        tiles = (recv_max + e_local * (TILE - 1)) // TILE
        part_w = ff // 2
        chips = ep // 2
        rows_blk = tok * SUB
        vm = pl.BlockSpec(memory_space=pltpu.VMEM)
        hbm = pl.BlockSpec(memory_space=pl.ANY)
        sm = pl.BlockSpec(memory_space=pltpu.SMEM)
        dma = pltpu.SemaphoreType.DMA
        i32 = jnp.int32
        groups = (ep, send_max)
        u0, u1, slot, src, first, last, te, gate = pl.pallas_call(
            functools.partial(plan_kernel, ep, tiles),
            out_shape=[
                jax.ShapeDtypeStruct((ep * tok, part_w), BF16),
                jax.ShapeDtypeStruct((width // part_w - 1, tok, part_w), BF16),
                jax.ShapeDtypeStruct((e_local, SUB, ep * tok), F32),
                jax.ShapeDtypeStruct(groups, i32),
                jax.ShapeDtypeStruct(groups, i32),
                jax.ShapeDtypeStruct((ep, tok), i32),
                jax.ShapeDtypeStruct((1, LANE), i32),
                jax.ShapeDtypeStruct(groups, F32),
            ],
            in_specs=[vm] * 4,
            out_specs=[vm] * 8,
            scratch_shapes=[
                pltpu.VMEM((w_router.shape[1], tok), F32),
                pltpu.VMEM((ep, top_k, tok), i32),
                pltpu.VMEM((ep, e_local, tok), F32),
                dma((2, ep)),
                dma((2, ep)),
                dma((14,)),
                dma((14,)),
            ],
            compiler_params=pltpu.CompilerParams(collective_id=0, has_side_effects=True),
            name="moe_plan",
        )(tokens, expert_ids.T, norm_gain, w_router.T)
        return pl.pallas_call(
            functools.partial(moe_kernel, ep, tiles),
            out_shape=jax.ShapeDtypeStruct((tok, width), BF16),
            in_specs=[sm] * 5 + [hbm, vm, vm, hbm, hbm, hbm, hbm],
            out_specs=vm,
            scratch_shapes=[
                pltpu.VMEM((width // part_w, ep * tok, part_w), BF16),
                pltpu.VMEM((tok, width), BF16),
                pltpu.VMEM((tiles * TILE, ff), BF16),
                *[pltpu.VMEM((e_local, part_w, part_w), BF16)] * 4,
                pltpu.VMEM((2 * chips * rows_blk, LANE), F32),
                pltpu.VMEM((2 * rows_blk, LANE), F32),
                pltpu.VMEM((4 * rows_blk + SUB, LANE), F32),
                dma((2,)),
                dma((4,)),
                dma((width // part_w, 14)),
                dma((width // part_w, 14)),
                dma((2, chips)),
                dma((2, chips)),
                dma((2, 2)),
                dma((2, 2)),
                dma((2, 4)),
                dma((2, 4)),
            ],
            compiler_params=pltpu.CompilerParams(
                collective_id=1, has_side_effects=True, vmem_limit_bytes=67_043_328),
            name="moe_block",
        )(te, src, first, last, gate, u0, u1, slot, tokens, w_gate, w_up, w_down)

    row_spec = P(("dp", "ep"), None)
    expert_spec = P("ep", None, None)
    return jax.shard_map(
        device_step, mesh=mesh,
        in_specs=(row_spec, row_spec, P(None), P(None, None), expert_spec, expert_spec, expert_spec),
        out_specs=row_spec, check_vma=False)
```

```python
import functools

import jax
import jax.numpy as jnp
from jax import lax
from jax.experimental import pallas as pl
from jax.experimental.pallas import tpu as pltpu
from jax.sharding import PartitionSpec as P

NORM_EPS = 1e-5
TILE = 128
SUB = 8
LANE = 128
F32 = jnp.float32
BF16 = jnp.bfloat16
MESH = pl.DeviceIdType.MESH


def dot(a, b, dims=(((1,), (0,)), ((), ()))):
    return lax.dot_general(a, b, dims, preferred_element_type=F32)


NT_DIMS = (((1,), (1,)), ((), ()))


class Place:
    def __init__(self, ep):
        self.ep = ep
        self.me = lax.axis_index("ep")
        self.xi, self.core = self.me // 2, self.me % 2
        self.chips = ep // 2
        self.right, self.left, self.far = self.dev(1, self.core), self.dev(-1, self.core), self.dev(2, self.core)
        self.partner = self.dev(0, 1 - self.core)

    def dev(self, dx, c):
        return lax.rem(self.xi + dx + self.chips, self.chips) * 2 + c

    def signal_all(self):
        barrier = pltpu.get_barrier_semaphore()
        for d in range(1, self.ep):
            pl.semaphore_signal(barrier, inc=1, device_id={"ep": lax.rem(self.me + d, self.ep)}, device_id_type=MESH)
        return barrier


class Gather:
    def __init__(self, pc, ref, send, recv, tok, own=None):
        self.pc, self.ref, self.send, self.recv, self.tok, self.own = pc, ref, send, recv, tok, own

    def copy(self, j, block, r, target, own=False):
        hr = self.tok // 2
        rows = pl.ds(pl.multiple_of(block * self.tok + r * hr, hr), hr)
        dst = self.ref.at[rows, :]
        src = self.own.at[pl.ds(r * hr, hr), :] if own and self.own is not None else dst
        return pltpu.make_async_remote_copy(
            src, dst, self.send.at[j], self.recv.at[j], device_id={"ep": target}, device_id_type=MESH)

    def start(self):
        p = self.pc
        self.copy(0, p.me, 0, p.right, True).start()
        self.copy(2, p.me, 1, p.left, True).start()
        self.copy(1, p.me, 1, p.right, True).start()
        self.copy(3, p.me, 0, p.left, True).start()
        self.copy(6, p.me, 0, p.partner, True).start()
        self.copy(7, p.me, 1, p.partner, True).start()

    def forward(self):
        p = self.pc
        self.copy(0, p.left, 0, p.right).wait_recv()
        self.copy(4, p.left, 0, p.right).start()
        self.copy(8, p.left, 0, p.partner).start()
        self.copy(2, p.right, 1, p.left).wait_recv()
        self.copy(5, p.right, 1, p.left).start()
        self.copy(11, p.right, 1, p.partner).start()

    def rest(self):
        p = self.pc
        self.copy(1, p.left, 1, p.right).wait_recv()
        self.copy(9, p.left, 1, p.partner).start()
        self.copy(3, p.right, 0, p.left).wait_recv()
        self.copy(10, p.right, 0, p.partner).start()

    def last(self):
        p = self.pc
        self.copy(4, p.far, 0, p.right).wait_recv()
        self.copy(12, p.far, 0, p.partner).start()
        self.copy(5, p.far, 1, p.left).wait_recv()
        self.copy(13, p.far, 1, p.partner).start()

    def finish(self):
        p = self.pc
        for j, (dx, r) in enumerate(((0, 0), (0, 1), (-1, 0), (-1, 1), (1, 0), (1, 1), (2, 0), (2, 1))):
            self.copy(6 + j, p.dev(dx, 1 - p.core), r, p.partner).wait_recv()

    def drain(self):
        for j in range(14):
            self.copy(j, self.pc.me, 0, self.pc.right).wait_send()


def plan_kernel(
    ep, tiles,
    x_hbm, ids_hbm, gain_hbm, wr_hbm,
    u0_ref, u1_ref, slot_ref, src_v, first_v, last_v, te_v, gate_v,
    x_ref, ids_ref, gain_ref, wr_ref, p_ref, id_land, p_land,
    in_sem, small_send, small_recv, ag_send, ag_recv,
):
    pc = Place(ep)
    me = pc.me
    ops_in = [pltpu.make_async_copy(a, b, in_sem.at[i]) for i, (a, b) in enumerate(
        ((x_hbm, x_ref), (gain_hbm, gain_ref), (wr_hbm, wr_ref), (ids_hbm, ids_ref)))]
    for c in ops_in:
        c.start()
    tok, width = x_ref.shape
    part_w = u0_ref.shape[1]
    e_local = slot_ref.shape[0]
    q_max = src_v.shape[0] * LANE // ep
    barrier = pc.signal_all()
    for c in ops_in:
        c.wait()

    x32 = x_ref[...].astype(F32)
    inv = lax.rsqrt(jnp.mean(x32 * x32, axis=1, keepdims=True) + NORM_EPS)
    u_own = (x32 * inv * gain_ref[...].astype(F32)[None, :]).astype(BF16)
    own_rows = pl.ds(pl.multiple_of(me * tok, tok), tok)
    u0_ref[own_rows, :] = u_own[:, :part_w]
    for k in range(1, width // part_w):
        u1_ref[k - 1] = u_own[:, k * part_w:(k + 1) * part_w]

    pl.semaphore_wait(barrier, ep - 1)

    ag = Gather(pc, u0_ref, ag_send, ag_recv, tok)
    ag.start()

    logits = dot(wr_ref[...], u_own, NT_DIMS)
    ex = jnp.exp(logits - jnp.max(logits, axis=0, keepdims=True))
    p_ref[...] = ex / jnp.sum(ex, axis=0, keepdims=True)
    id_land[me] = ids_ref[...]
    p_land[me] = p_ref[pl.ds(pl.multiple_of(me * e_local, e_local), e_local), :]

    def small(d, kind, target):
        if kind == 0:
            src, dst = ids_ref, id_land.at[me]
        else:
            src, dst = p_ref.at[pl.ds(pl.multiple_of(target * e_local, e_local), e_local), :], p_land.at[me]
        return pltpu.make_async_remote_copy(
            src, dst, small_send.at[kind, d], small_recv.at[kind, d], device_id={"ep": target}, device_id_type=MESH)

    for kind in range(2):
        for d in range(1, ep):
            small(d, kind, lax.rem(me + d, ep)).start()
    for kind in range(2):
        for d in range(1, ep):
            small(d, kind, lax.rem(me + d, ep)).wait_recv()

    base = me * e_local
    sub_i = lax.broadcasted_iota(jnp.int32, (e_local, LANE), 0)
    lane_i = lax.broadcasted_iota(jnp.int32, (e_local, LANE), 1)
    tri = (lax.broadcasted_iota(jnp.int32, (LANE, LANE), 0) < lax.broadcasted_iota(jnp.int32, (LANE, LANE), 1)).astype(BF16)
    member = []
    for b in range(ep):
        ids_b = id_land[b]
        m = jnp.zeros((e_local, LANE), F32)
        for k in range(ids_b.shape[0]):
            m = m + jnp.where(ids_b[k:k + 1, :] == base + sub_i, 1.0, 0.0)
        member.append(m)
    stack = jnp.concatenate(member, axis=0)
    before = dot(stack.astype(BF16), tri)
    total = jnp.sum(stack, axis=1, keepdims=True)
    run = jnp.zeros((e_local, 1), F32)
    pos = []
    for b in range(ep):
        pos.append(before[b * e_local:(b + 1) * e_local] + run)
        run = run + total[b * e_local:(b + 1) * e_local]
    tiles_e = jnp.floor((run + (TILE - 1)) * (1.0 / TILE))
    start = jnp.zeros((e_local, 1), F32)
    sub_c = lax.broadcasted_iota(jnp.int32, (e_local, 1), 0)
    for e in range(e_local):
        start = start + jnp.where(sub_c > e, tiles_e[e:e + 1, :], 0.0)
    tile_end = start + tiles_e
    te = jnp.sum(jnp.where(tile_end <= lane_i.astype(F32), 1.0, 0.0), axis=0, keepdims=True)
    te_v[...] = jnp.clip(te.astype(jnp.int32), 0, e_local - 1)
    count = jnp.concatenate([jnp.sum(m, axis=0, keepdims=True) for m in member], axis=0)
    first_rank = dot(count.astype(BF16), tri)
    last_row = jnp.where(count > 0, first_rank + count - 1.0, q_max * 1.0)
    last_v[...] = jnp.clip(last_row.astype(jnp.int32), 0, q_max)
    q_row = lax.broadcasted_iota(jnp.int32, (q_max, LANE), 0).astype(F32)
    q_lane = lax.broadcasted_iota(jnp.int32, (e_local, q_max), 1).astype(F32)
    for b in range(ep):
        m = member[b]
        slot = jnp.where(m > 0, start * TILE + pos[b], -1.0)
        slot_ref[:, :, b * LANE:(b + 1) * LANE] = jnp.broadcast_to(slot[:, None, :], (e_local, SUB, LANE))
        pre = jnp.zeros((e_local, LANE), F32)
        for e in range(e_local):
            pre = pre + jnp.where(sub_i > e, m[e:e + 1, :], 0.0)
        fr, ct = first_rank[b:b + 1], count[b:b + 1]
        rank = jnp.where(m > 0, fr + pre, 300.0)
        hi = jnp.floor(slot * (1.0 / 64))
        pb = p_land[b]
        g1 = pb.astype(BF16).astype(F32)
        g2 = (pb - g1).astype(BF16).astype(F32)
        g3 = pb - g1 - g2
        feats = jnp.concatenate([rank, hi, slot - hi * 64.0, jnp.broadcast_to(fr, m.shape), g1, g2, g3, pre], axis=0)
        hot = jnp.where((q_row >= fr) & (q_row < fr + ct), 1.0, 0.0).astype(BF16)
        got = dot(feats.astype(BF16), hot, NT_DIMS)
        e8 = e_local
        sel = got[0:e8] == q_lane
        src = jnp.sum(jnp.where(sel, got[e8:2 * e8] * 64.0 + got[2 * e8:3 * e8], 0.0), axis=0, keepdims=True)
        gate = jnp.sum(jnp.where(sel, got[4 * e8:5 * e8] + got[5 * e8:6 * e8] + got[6 * e8:7 * e8], 0.0), axis=0, keepdims=True)
        src = jnp.clip(src.astype(jnp.int32), 0, tiles * TILE - 1)
        first = (got[3 * e8:3 * e8 + 1] == q_lane[0:1]).astype(jnp.int32)
        for v in range(q_max // LANE):
            r, lanes = b * (q_max // LANE) + v, slice(v * LANE, (v + 1) * LANE)
            src_v[r:r + 1, :] = src[:, lanes]
            first_v[r:r + 1, :] = first[:, lanes]
            gate_v[r:r + 1, :] = gate[:, lanes]

    ag.forward()
    ag.rest()
    ag.last()
    ag.finish()
    ag.drain()
    for kind in range(2):
        for d in range(1, ep):
            small(d, kind, lax.rem(me + d, ep)).wait_send()


def moe_kernel(
    ep, tiles,
    te_hbm, src_hbm, first_hbm, last_hbm, gate_hbm,
    u0_hbm, u1_hbm, slot_hbm, x_hbm, w1_hbm, w3_hbm, w2_hbm,
    out_ref,
    te_s, src_s, first_s, last_s, gate_s, u1_ref, slot_ref,
    u_all, x_v, h_ref, ring0, ring1, ring2, ring3,
    recv_a, recv_h, recv_d,
    in_sem, ring_sem, ag_send, ag_recv,
    a_send, a_recv, h_send, h_recv, d_send, d_recv,
):
    pc = Place(ep)
    me, core, chips, dev = pc.me, pc.core, pc.chips, pc.dev
    right, left, partner, far = pc.right, pc.left, pc.partner, pc.far
    ring = (ring0, ring1, ring2, ring3)
    tok, width = x_v.shape
    q_max = src_s.shape[0] // ep
    half_w = width // 2
    part_w = ring0.shape[1]
    parts = width // part_w
    rows_blk = tok * SUB

    def up_copy(k, m):
        w = (w1_hbm, w3_hbm)[m % 2]
        rows = pl.ds(pl.multiple_of(k * part_w, part_w), part_w)
        return pltpu.make_async_copy(w.at[:, rows, pl.ds(m // 2 * part_w, part_w)], ring[m], ring_sem.at[m])

    def w2_copy(q, m):
        rows = pl.ds(m % 2 * part_w, part_w)
        return pltpu.make_async_copy(w2_hbm.at[:, rows, pl.ds((2 * q + m // 2) * part_w, part_w)], ring[m], ring_sem.at[m])

    barrier = pc.signal_all()
    pairs_in = ((u1_hbm, u1_ref), (u0_hbm, u_all.at[0]), (te_hbm, te_s), (slot_hbm, slot_ref), (src_hbm, src_s),
                (first_hbm, first_s), (last_hbm, last_s), (gate_hbm, gate_s), (x_hbm, x_v))
    ops_in = [pltpu.make_async_copy(a, b, in_sem.at[i]) for i, (a, b) in enumerate(pairs_in)]
    for c in ops_in[:4]:
        c.start()
    for m in range(4):
        up_copy(0, m).start()
    for c in ops_in[4:]:
        c.start()
    own_rows = pl.ds(pl.multiple_of(me * tok, tok), tok)
    ops_in[0].wait()
    for k in range(1, parts):
        u_all[k, own_rows, :] = u1_ref[k - 1]
    pl.semaphore_wait(barrier, ep - 1)

    def ag(k):
        return Gather(pc, u_all.at[k], ag_send.at[k], ag_recv.at[k], tok, own=u1_ref.at[k - 1])

    ag(1).start()
    for c in ops_in[1:4]:
        c.wait()

    def tile_expert(i):
        return te_s[0, i]

    def phase_one(ug, acc):
        t_iota = lax.broadcasted_iota(jnp.int32, (TILE, ep * tok), 0).astype(F32)

        def gather(k):
            def tile(i):
                row = slot_ref[tile_expert(i)][0:1] - lax.convert_element_type(i * TILE, F32)
                hot = jnp.where(row == t_iota, 1.0, 0.0).astype(BF16)
                ug[pl.ds(pl.multiple_of(i * TILE, TILE), TILE), :] = dot(hot, u_all[k]).astype(BF16)

            un = 6
            whole = tiles // un

            def body(g, carry):
                for j in range(un):
                    tile(g * un + j)
                return carry

            lax.fori_loop(0, whole, body, 0)
            for i in range(whole * un, tiles):
                tile(jnp.int32(i))

        def slice_dots(k, m, final):
            fs, which = m // 2, m % 2
            up_copy(k, m).wait()
            for i in range(tiles):
                rows = pl.ds(i * TILE, TILE)
                d = dot(ug[rows, :], ring[m][tile_expert(i)])
                if not final:
                    acc[which, fs, rows, :] = jnp.where(k == 0, 0.0, acc[which, fs, rows, :]) + d
                elif which == 0:
                    acc[0, fs, rows, :] = acc[0, fs, rows, :] + d
                else:
                    g = acc[0, fs, rows, :]
                    h_ref[rows, fs * part_w:(fs + 1) * part_w] = (
                        g / (1.0 + jnp.exp(-g)) * (acc[1, fs, rows, :] + d)).astype(BF16)

        def part(k, carry):
            nxt = ag(k + 1)
            gather(k)

            def pass_on():
                nxt.forward()

                @pl.when(k < parts - 2)
                def _():
                    ag(k + 2).start()

            pl.when(k > 0)(pass_on)
            for m in range(4):
                slice_dots(k, m, False)
                up_copy(k + 1, m).start()
                if m == 0:
                    pl.when(k == 0)(pass_on)
                elif m == 1:
                    nxt.rest()
                elif m == 2:
                    pl.when(k > 0)(nxt.last)
                else:
                    pl.when(k == 0)(nxt.last)
            nxt.finish()
            return carry

        lax.fori_loop(0, parts - 1, part, 0)
        gather(parts - 1)
        for m in range(4):
            slice_dots(parts - 1, m, True)
            w2_copy(0, m).start()

    pl.run_scoped(
        phase_one,
        pltpu.VMEM((tiles * TILE, part_w), BF16),
        pltpu.VMEM((2, 2, tiles * TILE, part_w), F32),
    )

    def phase_two(o3, pbuf, accb):
        order = (2, 1, 3, 0)
        o_rows = o3.reshape(o3.shape[0] // SUB, SUB, LANE)
        p_rows = pbuf.reshape(pbuf.shape[0] // SUB, SUB, LANE)
        pbuf[q_max * SUB:(q_max + 1) * SUB, :] = jnp.zeros((SUB, LANE), F32)

        def block(q, s):
            return pl.ds(pl.multiple_of((q * ep + s) * rows_blk, rows_blk), rows_blk)

        def combine(q, s):
            un = 16

            def pairs(i, run):
                at = s * q_max + i * un
                for j in range(un):
                    row = o_rows[src_s[at + j]]
                    is_first = jnp.full((SUB, LANE), first_s[at + j], jnp.int32) == 1
                    run = jnp.where(is_first, 0.0, run) + gate_s[at + j] * row
                    pbuf[pl.ds(pl.multiple_of((i * un + j) * SUB, SUB), SUB), :] = run
                return run

            lax.fori_loop(0, q_max // un, pairs, jnp.zeros((SUB, LANE), F32))

            def tokens(i, carry):
                at = s * tok + i * un
                for j in range(un):
                    dst = pl.ds(pl.multiple_of((q * ep + s) * rows_blk + (i * un + j) * SUB, SUB), SUB)
                    accb[dst, :] = p_rows[last_s[at + j]]
                return carry

            lax.fori_loop(0, tok // un, tokens, 0)

        def a_copy(q, j):
            rows = pl.ds((q * chips + j) * rows_blk, rows_blk)
            return pltpu.make_async_remote_copy(
                accb.at[block(q, dev(order[j], 1 - core)), :], recv_a.at[rows, :], a_send.at[q, j], a_recv.at[q, j],
                device_id={"ep": partner}, device_id_type=MESH)

        def a_add(q, j):
            a_copy(q, j).wait_recv()
            mine = block(q, dev(order[j], core))
            accb[mine, :] = accb[mine, :] + recv_a[(q * chips + j) * rows_blk:(q * chips + j + 1) * rows_blk, :]

        hb = rows_blk // 2

        def half(q, s, r):
            return pl.ds(pl.multiple_of((q * ep + s) * rows_blk + r * hb, hb), hb)

        def h_copy(q, side):
            return pltpu.make_async_remote_copy(
                accb.at[half(q, far, side), :], recv_h.at[pl.ds((q * 2 + side) * hb, hb), :], h_send.at[q, side], h_recv.at[q, side],
                device_id={"ep": left if side else right}, device_id_type=MESH)

        def d_copy(q, side, r):
            s = left if side else right
            return pltpu.make_async_remote_copy(
                accb.at[half(q, s, r), :], recv_d.at[pl.ds((q * 2 + side) * rows_blk + r * hb, hb), :],
                d_send.at[q, side * 2 + r], d_recv.at[q, side * 2 + r], device_id={"ep": s}, device_id_type=MESH)

        def relay(q):
            for side in range(2):
                h_copy(q, side).wait_recv()
                s = left if side else right
                mine = half(q, s, side)
                accb[mine, :] = accb[mine, :] + recv_h[(q * 2 + side) * hb:(q * 2 + side + 1) * hb, :]
                d_copy(q, side, side).start()

        def down(q):
            lanes = part_w // LANE
            for g in range(2):
                w2_copy(q, 2 * g).wait()
                w2_copy(q, 2 * g + 1).wait()
                for i in range(tiles):
                    rows = slice(i * TILE, (i + 1) * TILE)
                    e = tile_expert(i)
                    o = dot(h_ref[rows, :part_w], ring[2 * g][e]) + dot(h_ref[rows, part_w:], ring[2 * g + 1][e])
                    o = o.astype(BF16).astype(F32)
                    for v in range(lanes):
                        o3[pl.ds(i * TILE * SUB + g * lanes + v, TILE, stride=SUB), :] = o[:, v * LANE:(v + 1) * LANE]
                if q == 0:
                    w2_copy(1, 2 * g).start()
                    w2_copy(1, 2 * g + 1).start()
                elif g == 0:
                    relay(0)

        def scatter(q):
            def settle(j):
                a_add(q, j)
                if j == 0:
                    h_copy(q, 0).start()
                    h_copy(q, 1).start()
                elif j == 1:
                    d_copy(q, 0, 1).start()
                elif j == 2:
                    d_copy(q, 1, 0).start()

            for j in range(chips):
                combine(q, dev(order[j], 1 - core))
                a_copy(q, j).start()
                combine(q, dev(order[j], core))
                if j > 0:
                    settle(j - 1)
            settle(chips - 1)

        def finish(q):
            for side in range(2):
                for r in range(2):
                    d_copy(q, side, r).wait_recv()
            for v in range(half_w // LANE):
                cols = slice(q * half_w + v * LANE, q * half_w + (v + 1) * LANE)
                own = accb[pl.ds((q * ep + me) * rows_blk + v, tok, stride=SUB), :]
                d0 = recv_d[pl.ds(q * 2 * rows_blk + v, tok, stride=SUB), :]
                d1 = recv_d[pl.ds((q * 2 + 1) * rows_blk + v, tok, stride=SUB), :]
                out_ref[:, cols] = (x_v[:, cols].astype(F32) + (own + d0 + d1)).astype(BF16)

        down(0)
        for c in ops_in[4:8]:
            c.wait()
        scatter(0)
        down(1)
        scatter(1)
        relay(1)
        ops_in[8].wait()
        finish(0)
        finish(1)
        for q in range(2):
            for j in range(chips):
                a_copy(q, j).wait_send()
            for side in range(2):
                h_copy(q, side).wait_send()
                for r in range(2):
                    d_copy(q, side, r).wait_send()

    pl.run_scoped(
        phase_two,
        pltpu.VMEM((tiles * TILE * SUB + SUB, LANE), F32),
        pltpu.VMEM(((q_max + 1) * SUB, LANE), F32),
        pltpu.VMEM((2 * ep * rows_blk + SUB, LANE), F32),
    )

    for k in range(1, parts):
        ag(k).drain()


def solution(mesh):
    ep = mesh.shape["ep"]

    def device_step(tokens, expert_ids, norm_gain, w_router, w_gate, w_up, w_down):
        tok, top_k = expert_ids.shape
        width = tokens.shape[1]
        e_local, _, ff = w_gate.shape
        pairs = tok * top_k
        send_max = 2 * pairs // ep
        recv_max = 3 * pairs // 2
        tiles = (recv_max + e_local * (TILE - 1)) // TILE
        part_w = ff // 2
        chips = ep // 2
        rows_blk = tok * SUB
        vm = pl.BlockSpec(memory_space=pltpu.VMEM)
        hbm = pl.BlockSpec(memory_space=pl.ANY)
        dma = pltpu.SemaphoreType.DMA
        i32 = jnp.int32
        groups = (ep * send_max // LANE, LANE)
        u0, u1, slot, src, first, last, te, gate = pl.pallas_call(
            functools.partial(plan_kernel, ep, tiles),
            out_shape=[
                jax.ShapeDtypeStruct((ep * tok, part_w), BF16),
                jax.ShapeDtypeStruct((width // part_w - 1, tok, part_w), BF16),
                jax.ShapeDtypeStruct((e_local, SUB, ep * tok), F32),
                jax.ShapeDtypeStruct(groups, i32),
                jax.ShapeDtypeStruct(groups, i32),
                jax.ShapeDtypeStruct((ep, tok), i32),
                jax.ShapeDtypeStruct((1, LANE), i32),
                jax.ShapeDtypeStruct(groups, F32),
            ],
            in_specs=[hbm] * 4,
            out_specs=[vm] * 8,
            scratch_shapes=[
                pltpu.VMEM((tok, width), BF16),
                pltpu.VMEM((top_k, tok), i32),
                pltpu.VMEM((width,), BF16),
                pltpu.VMEM((w_router.shape[1], width), BF16),
                pltpu.VMEM((w_router.shape[1], tok), F32),
                pltpu.VMEM((ep, top_k, tok), i32),
                pltpu.VMEM((ep, e_local, tok), F32),
                dma((4,)),
                dma((2, ep)),
                dma((2, ep)),
                dma((14,)),
                dma((14,)),
            ],
            compiler_params=pltpu.CompilerParams(collective_id=0, has_side_effects=True),
            name="moe_plan",
        )(tokens, expert_ids.T, norm_gain, w_router.T)
        return pl.pallas_call(
            functools.partial(moe_kernel, ep, tiles),
            out_shape=jax.ShapeDtypeStruct((tok, width), BF16),
            in_specs=[hbm] * 12,
            out_specs=vm,
            scratch_shapes=[
                pltpu.SMEM((1, LANE), i32),
                pltpu.SMEM((ep * send_max,), i32),
                pltpu.SMEM((ep * send_max,), i32),
                pltpu.SMEM((ep * tok,), i32),
                pltpu.SMEM((ep * send_max,), F32),
                pltpu.VMEM((width // part_w - 1, tok, part_w), BF16),
                pltpu.VMEM((e_local, SUB, ep * tok), F32),
                pltpu.VMEM((width // part_w, ep * tok, part_w), BF16),
                pltpu.VMEM((tok, width), BF16),
                pltpu.VMEM((tiles * TILE, ff), BF16),
                *[pltpu.VMEM((e_local, part_w, part_w), BF16)] * 4,
                pltpu.VMEM((2 * chips * rows_blk, LANE), F32),
                pltpu.VMEM((2 * rows_blk, LANE), F32),
                pltpu.VMEM((4 * rows_blk + SUB, LANE), F32),
                dma((9,)),
                dma((4,)),
                dma((width // part_w, 14)),
                dma((width // part_w, 14)),
                dma((2, chips)),
                dma((2, chips)),
                dma((2, 2)),
                dma((2, 2)),
                dma((2, 4)),
                dma((2, 4)),
            ],
            compiler_params=pltpu.CompilerParams(
                collective_id=1, has_side_effects=True, vmem_limit_bytes=67_043_328),
            name="moe_block",
        )(te, src.reshape(-1), first.reshape(-1), last.reshape(-1), gate.reshape(-1), u0, u1, slot, tokens, w_gate, w_up, w_down)

    row_spec = P(("dp", "ep"), None)
    expert_spec = P("ep", None, None)
    return jax.shard_map(
        device_step, mesh=mesh,
        in_specs=(row_spec, row_spec, P(None), P(None, None), expert_spec, expert_spec, expert_spec),
        out_specs=row_spec, check_vma=False)
```

```python
import functools

import jax
import jax.numpy as jnp
from jax import lax
from jax.experimental import pallas as pl
from jax.experimental.pallas import tpu as pltpu
from jax.sharding import PartitionSpec as P

NORM_EPS = 1e-5
TILE = 128
SUB = 8
LANE = 128
F32 = jnp.float32
BF16 = jnp.bfloat16
MESH = pl.DeviceIdType.MESH


def dot(a, b, dims=(((1,), (0,)), ((), ()))):
    return lax.dot_general(a, b, dims, preferred_element_type=F32)


NT_DIMS = (((1,), (1,)), ((), ()))


class Place:
    def __init__(self, ep):
        self.ep = ep
        self.me = lax.axis_index("ep")
        self.xi, self.core = self.me // 2, self.me % 2
        self.chips = ep // 2
        self.right, self.left, self.far = self.dev(1, self.core), self.dev(-1, self.core), self.dev(2, self.core)
        self.partner = self.dev(0, 1 - self.core)

    def dev(self, dx, c):
        return lax.rem(self.xi + dx + self.chips, self.chips) * 2 + c

    def signal_all(self):
        barrier = pltpu.get_barrier_semaphore()
        for d in range(1, self.ep):
            pl.semaphore_signal(barrier, inc=1, device_id={"ep": lax.rem(self.me + d, self.ep)}, device_id_type=MESH)
        return barrier


class Gather:
    def __init__(self, pc, ref, send, recv, tok, own=None):
        self.pc, self.ref, self.send, self.recv, self.tok, self.own = pc, ref, send, recv, tok, own

    def copy(self, j, block, r, target, own=False):
        hr = self.tok // 2
        rows = pl.ds(pl.multiple_of(block * self.tok + r * hr, hr), hr)
        dst = self.ref.at[rows, :]
        src = self.own.at[pl.ds(r * hr, hr), :] if own and self.own is not None else dst
        return pltpu.make_async_remote_copy(
            src, dst, self.send.at[j], self.recv.at[j], device_id={"ep": target}, device_id_type=MESH)

    def start(self):
        p = self.pc
        self.copy(0, p.me, 0, p.right, True).start()
        self.copy(2, p.me, 1, p.left, True).start()
        self.copy(1, p.me, 1, p.right, True).start()
        self.copy(3, p.me, 0, p.left, True).start()
        self.copy(6, p.me, 0, p.partner, True).start()
        self.copy(7, p.me, 1, p.partner, True).start()

    def forward(self):
        p = self.pc
        self.copy(0, p.left, 0, p.right).wait_recv()
        self.copy(4, p.left, 0, p.right).start()
        self.copy(8, p.left, 0, p.partner).start()
        self.copy(2, p.right, 1, p.left).wait_recv()
        self.copy(5, p.right, 1, p.left).start()
        self.copy(11, p.right, 1, p.partner).start()

    def rest(self):
        p = self.pc
        self.copy(1, p.left, 1, p.right).wait_recv()
        self.copy(9, p.left, 1, p.partner).start()
        self.copy(3, p.right, 0, p.left).wait_recv()
        self.copy(10, p.right, 0, p.partner).start()

    def last(self):
        p = self.pc
        self.copy(4, p.far, 0, p.right).wait_recv()
        self.copy(12, p.far, 0, p.partner).start()
        self.copy(5, p.far, 1, p.left).wait_recv()
        self.copy(13, p.far, 1, p.partner).start()

    def finish(self):
        p = self.pc
        for j, (dx, r) in enumerate(((0, 0), (0, 1), (-1, 0), (-1, 1), (1, 0), (1, 1), (2, 0), (2, 1))):
            self.copy(6 + j, p.dev(dx, 1 - p.core), r, p.partner).wait_recv()

    def drain(self):
        for j in range(14):
            self.copy(j, self.pc.me, 0, self.pc.right).wait_send()


def plan_kernel(
    ep, tiles,
    x_hbm, ids_hbm, gain_hbm, wr_hbm,
    u0_ref, u1_ref, slot_ref, src_v, first_v, last_v, te_v, gate_v,
    x_ref, ids_ref, gain_ref, wr_ref, p_ref, id_land, p_land,
    in_sem, small_send, small_recv, ag_send, ag_recv,
):
    pc = Place(ep)
    me = pc.me
    ops_in = [pltpu.make_async_copy(a, b, in_sem.at[i]) for i, (a, b) in enumerate(
        ((x_hbm, x_ref), (gain_hbm, gain_ref), (wr_hbm, wr_ref), (ids_hbm, ids_ref)))]
    for c in ops_in:
        c.start()
    tok, width = x_ref.shape
    part_w = u0_ref.shape[1]
    e_local = slot_ref.shape[0]
    q_max = src_v.shape[0] * LANE // ep
    barrier = pc.signal_all()
    for c in ops_in:
        c.wait()

    x32 = x_ref[...].astype(F32)
    inv = lax.rsqrt(jnp.mean(x32 * x32, axis=1, keepdims=True) + NORM_EPS)
    u_own = (x32 * inv * gain_ref[...].astype(F32)[None, :]).astype(BF16)
    own_rows = pl.ds(pl.multiple_of(me * tok, tok), tok)
    u0_ref[own_rows, :] = u_own[:, :part_w]
    for k in range(1, width // part_w):
        u1_ref[k - 1] = u_own[:, k * part_w:(k + 1) * part_w]

    pl.semaphore_wait(barrier, ep - 1)

    ag = Gather(pc, u0_ref, ag_send, ag_recv, tok)
    ag.start()

    logits = dot(wr_ref[...], u_own, NT_DIMS)
    ex = jnp.exp(logits - jnp.max(logits, axis=0, keepdims=True))
    p_ref[...] = ex / jnp.sum(ex, axis=0, keepdims=True)
    id_land[me] = ids_ref[...]
    p_land[me] = p_ref[pl.ds(pl.multiple_of(me * e_local, e_local), e_local), :]

    def small(d, kind, target):
        if kind == 0:
            src, dst = ids_ref, id_land.at[me]
        else:
            src, dst = p_ref.at[pl.ds(pl.multiple_of(target * e_local, e_local), e_local), :], p_land.at[me]
        return pltpu.make_async_remote_copy(
            src, dst, small_send.at[kind, d], small_recv.at[kind, d], device_id={"ep": target}, device_id_type=MESH)

    for kind in range(2):
        for d in range(1, ep):
            small(d, kind, lax.rem(me + d, ep)).start()
    for kind in range(2):
        for d in range(1, ep):
            small(d, kind, lax.rem(me + d, ep)).wait_recv()

    base = me * e_local
    sub_i = lax.broadcasted_iota(jnp.int32, (e_local, LANE), 0)
    lane_i = lax.broadcasted_iota(jnp.int32, (e_local, LANE), 1)
    tri = (lax.broadcasted_iota(jnp.int32, (LANE, LANE), 0) < lax.broadcasted_iota(jnp.int32, (LANE, LANE), 1)).astype(BF16)
    member = []
    for b in range(ep):
        ids_b = id_land[b]
        m = jnp.zeros((e_local, LANE), F32)
        for k in range(ids_b.shape[0]):
            m = m + jnp.where(ids_b[k:k + 1, :] == base + sub_i, 1.0, 0.0)
        member.append(m)
    stack = jnp.concatenate(member, axis=0)
    before = dot(stack.astype(BF16), tri)
    total = jnp.sum(stack, axis=1, keepdims=True)
    run = jnp.zeros((e_local, 1), F32)
    pos = []
    for b in range(ep):
        pos.append(before[b * e_local:(b + 1) * e_local] + run)
        run = run + total[b * e_local:(b + 1) * e_local]
    tiles_e = jnp.floor((run + (TILE - 1)) * (1.0 / TILE))
    start = jnp.zeros((e_local, 1), F32)
    sub_c = lax.broadcasted_iota(jnp.int32, (e_local, 1), 0)
    for e in range(e_local):
        start = start + jnp.where(sub_c > e, tiles_e[e:e + 1, :], 0.0)
    tile_end = start + tiles_e
    te = jnp.sum(jnp.where(tile_end <= lane_i.astype(F32), 1.0, 0.0), axis=0, keepdims=True)
    te_v[...] = jnp.clip(te.astype(jnp.int32), 0, e_local - 1)
    count = jnp.concatenate([jnp.sum(m, axis=0, keepdims=True) for m in member], axis=0)
    first_rank = dot(count.astype(BF16), tri)
    last_row = jnp.where(count > 0, first_rank + count - 1.0, q_max * 1.0)
    last_v[...] = jnp.clip(last_row.astype(jnp.int32), 0, q_max)
    q_row = lax.broadcasted_iota(jnp.int32, (q_max, LANE), 0).astype(F32)
    q_lane = lax.broadcasted_iota(jnp.int32, (e_local, q_max), 1).astype(F32)
    for b in range(ep):
        m = member[b]
        slot = jnp.where(m > 0, start * TILE + pos[b], -1.0)
        slot_ref[:, :, b * LANE:(b + 1) * LANE] = jnp.broadcast_to(slot[:, None, :], (e_local, SUB, LANE))
        pre = jnp.zeros((e_local, LANE), F32)
        for e in range(e_local):
            pre = pre + jnp.where(sub_i > e, m[e:e + 1, :], 0.0)
        fr, ct = first_rank[b:b + 1], count[b:b + 1]
        rank = jnp.where(m > 0, fr + pre, 300.0)
        hi = jnp.floor(slot * (1.0 / 64))
        pb = p_land[b]
        g1 = pb.astype(BF16).astype(F32)
        g2 = (pb - g1).astype(BF16).astype(F32)
        g3 = pb - g1 - g2
        feats = jnp.concatenate([rank, hi, slot - hi * 64.0, jnp.broadcast_to(fr, m.shape), g1, g2, g3, pre], axis=0)
        hot = jnp.where((q_row >= fr) & (q_row < fr + ct), 1.0, 0.0).astype(BF16)
        got = dot(feats.astype(BF16), hot, NT_DIMS)
        e8 = e_local
        sel = got[0:e8] == q_lane
        src = jnp.sum(jnp.where(sel, got[e8:2 * e8] * 64.0 + got[2 * e8:3 * e8], 0.0), axis=0, keepdims=True)
        gate = jnp.sum(jnp.where(sel, got[4 * e8:5 * e8] + got[5 * e8:6 * e8] + got[6 * e8:7 * e8], 0.0), axis=0, keepdims=True)
        src = jnp.clip(src.astype(jnp.int32), 0, tiles * TILE - 1)
        first = (got[3 * e8:3 * e8 + 1] == q_lane[0:1]).astype(jnp.int32)
        for v in range(q_max // LANE):
            r, lanes = b * (q_max // LANE) + v, slice(v * LANE, (v + 1) * LANE)
            src_v[r:r + 1, :] = src[:, lanes]
            first_v[r:r + 1, :] = first[:, lanes]
            gate_v[r:r + 1, :] = gate[:, lanes]

    ag.forward()
    ag.rest()
    ag.last()
    ag.finish()
    ag.drain()
    for kind in range(2):
        for d in range(1, ep):
            small(d, kind, lax.rem(me + d, ep)).wait_send()


def moe_kernel(
    ep, tiles,
    te_hbm, src_hbm, first_hbm, last_hbm, gate_hbm,
    u0_hbm, u1_hbm, slot_hbm, x_hbm, w1_hbm, w3_hbm, w2_hbm,
    out_ref,
    te_s, src_s, first_s, last_s, gate_s, u1_ref, slot_ref,
    u_all, x_v, h_ref, ring0, ring1, ring2, ring3,
    recv_a, recv_h, recv_d,
    in_sem, ring_sem, ag_send, ag_recv,
    a_send, a_recv, h_send, h_recv, d_send, d_recv,
):
    pc = Place(ep)
    me, core, chips, dev = pc.me, pc.core, pc.chips, pc.dev
    right, left, partner, far = pc.right, pc.left, pc.partner, pc.far
    ring = (ring0, ring1, ring2, ring3)
    tok, width = x_v.shape
    q_max = src_s.shape[0] // ep
    half_w = width // 2
    part_w = ring0.shape[1]
    parts = width // part_w
    rows_blk = tok * SUB

    def up_copy(k, m):
        w = (w1_hbm, w3_hbm)[m % 2]
        rows = pl.ds(pl.multiple_of(k * part_w, part_w), part_w)
        return pltpu.make_async_copy(w.at[:, rows, pl.ds(m // 2 * part_w, part_w)], ring[m], ring_sem.at[m])

    def w2_copy(q, m):
        rows = pl.ds(m % 2 * part_w, part_w)
        return pltpu.make_async_copy(w2_hbm.at[:, rows, pl.ds((2 * q + m // 2) * part_w, part_w)], ring[m], ring_sem.at[m])

    barrier = pc.signal_all()
    pairs_in = ((u1_hbm, u1_ref), (u0_hbm, u_all.at[0]), (te_hbm, te_s), (slot_hbm, slot_ref), (src_hbm, src_s),
                (first_hbm, first_s), (last_hbm, last_s), (gate_hbm, gate_s), (x_hbm, x_v))
    ops_in = [pltpu.make_async_copy(a, b, in_sem.at[i]) for i, (a, b) in enumerate(pairs_in)]
    for c in ops_in[:4]:
        c.start()
    for m in range(4):
        up_copy(0, m).start()
    for c in ops_in[4:]:
        c.start()
    own_rows = pl.ds(pl.multiple_of(me * tok, tok), tok)
    ops_in[0].wait()
    for k in range(1, parts):
        u_all[k, own_rows, :] = u1_ref[k - 1]
    pl.semaphore_wait(barrier, ep - 1)

    def ag(k):
        return Gather(pc, u_all.at[k], ag_send.at[k], ag_recv.at[k], tok, own=u1_ref.at[k - 1])

    ag(1).start()
    for c in ops_in[1:4]:
        c.wait()

    def tile_expert(i):
        return te_s[0, i]

    def phase_one(ug, acc):
        t_iota = lax.broadcasted_iota(jnp.int32, (TILE, ep * tok), 0).astype(F32)

        def gather(k):
            def tile(i):
                row = slot_ref[tile_expert(i)][0:1] - float(i * TILE)
                hot = jnp.where(row == t_iota, 1.0, 0.0).astype(BF16)
                ug[i * TILE:(i + 1) * TILE, :] = dot(hot, u_all[k]).astype(BF16)

            for i in range(tiles):
                tile(i)

        def slice_dots(k, m, final):
            fs, which = m // 2, m % 2
            if not final:
                up_copy(k, m).wait()
            for i in range(tiles):
                rows = pl.ds(i * TILE, TILE)
                d = dot(ug[rows, :], ring[m][tile_expert(i)])
                if not final:
                    acc[which, fs, rows, :] = jnp.where(k == 0, 0.0, acc[which, fs, rows, :]) + d
                elif which == 0:
                    acc[0, fs, rows, :] = acc[0, fs, rows, :] + d
                else:
                    g = acc[0, fs, rows, :]
                    h_ref[rows, fs * part_w:(fs + 1) * part_w] = (
                        g / (1.0 + jnp.exp(-g)) * (acc[1, fs, rows, :] + d)).astype(BF16)

        def part(k, carry):
            nxt = ag(k + 1)
            gather(k)

            def pass_on():
                nxt.forward()

                @pl.when(k < parts - 2)
                def _():
                    ag(k + 2).start()

            pl.when(k > 0)(pass_on)
            for m in range(4):
                slice_dots(k, m, False)
                up_copy(k + 1, m).start()
                if m == 0:
                    pl.when(k == 0)(pass_on)
                elif m == 1:
                    nxt.rest()
                elif m == 2:
                    pl.when(k > 0)(nxt.last)
                else:
                    pl.when(k == 0)(nxt.last)
            nxt.finish()
            return carry

        lax.fori_loop(0, parts - 1, part, 0)
        gather(parts - 1)
        for m in range(4):
            up_copy(parts - 1, m).wait()
        for m in range(4):
            slice_dots(parts - 1, m, True)
            w2_copy(0, m).start()

    pl.run_scoped(
        phase_one,
        pltpu.VMEM((tiles * TILE, part_w), BF16),
        pltpu.VMEM((2, 2, tiles * TILE, part_w), F32),
    )

    def phase_two(o3, pbuf, accb):
        order = (2, 1, 3, 0)
        o_rows = o3.reshape(o3.shape[0] // SUB, SUB, LANE)
        p_rows = pbuf.reshape(pbuf.shape[0] // SUB, SUB, LANE)
        pbuf[q_max * SUB:(q_max + 1) * SUB, :] = jnp.zeros((SUB, LANE), F32)

        def block(q, s):
            return pl.ds(pl.multiple_of((q * ep + s) * rows_blk, rows_blk), rows_blk)

        def combine(q, s):
            un = 16

            def pairs(i, run):
                at = s * q_max + i * un
                for j in range(un):
                    row = o_rows[src_s[at + j]]
                    is_first = jnp.full((SUB, LANE), first_s[at + j], jnp.int32) == 1
                    run = jnp.where(is_first, 0.0, run) + gate_s[at + j] * row
                    pbuf[pl.ds(pl.multiple_of((i * un + j) * SUB, SUB), SUB), :] = run
                return run

            lax.fori_loop(0, q_max // un, pairs, jnp.zeros((SUB, LANE), F32))

            def tokens(i, carry):
                at = s * tok + i * un
                for j in range(un):
                    dst = pl.ds(pl.multiple_of((q * ep + s) * rows_blk + (i * un + j) * SUB, SUB), SUB)
                    accb[dst, :] = p_rows[last_s[at + j]]
                return carry

            lax.fori_loop(0, tok // un, tokens, 0)

        def a_copy(q, j):
            rows = pl.ds((q * chips + j) * rows_blk, rows_blk)
            return pltpu.make_async_remote_copy(
                accb.at[block(q, dev(order[j], 1 - core)), :], recv_a.at[rows, :], a_send.at[q, j], a_recv.at[q, j],
                device_id={"ep": partner}, device_id_type=MESH)

        def a_add(q, j):
            a_copy(q, j).wait_recv()
            mine = block(q, dev(order[j], core))
            accb[mine, :] = accb[mine, :] + recv_a[(q * chips + j) * rows_blk:(q * chips + j + 1) * rows_blk, :]

        hb = rows_blk // 2

        def half(q, s, r):
            return pl.ds(pl.multiple_of((q * ep + s) * rows_blk + r * hb, hb), hb)

        def h_copy(q, side):
            return pltpu.make_async_remote_copy(
                accb.at[half(q, far, side), :], recv_h.at[pl.ds((q * 2 + side) * hb, hb), :], h_send.at[q, side], h_recv.at[q, side],
                device_id={"ep": left if side else right}, device_id_type=MESH)

        def d_copy(q, side, r):
            s = left if side else right
            return pltpu.make_async_remote_copy(
                accb.at[half(q, s, r), :], recv_d.at[pl.ds((q * 2 + side) * rows_blk + r * hb, hb), :],
                d_send.at[q, side * 2 + r], d_recv.at[q, side * 2 + r], device_id={"ep": s}, device_id_type=MESH)

        def relay(q):
            for side in range(2):
                h_copy(q, side).wait_recv()
                s = left if side else right
                mine = half(q, s, side)
                accb[mine, :] = accb[mine, :] + recv_h[(q * 2 + side) * hb:(q * 2 + side + 1) * hb, :]
                d_copy(q, side, side).start()

        def down(q):
            lanes = part_w // LANE
            for g in range(2):
                w2_copy(q, 2 * g).wait()
                w2_copy(q, 2 * g + 1).wait()
                for i in range(tiles):
                    rows = slice(i * TILE, (i + 1) * TILE)
                    e = tile_expert(i)
                    o = dot(h_ref[rows, :part_w], ring[2 * g][e]) + dot(h_ref[rows, part_w:], ring[2 * g + 1][e])
                    o = o.astype(BF16).astype(F32)
                    for v in range(lanes):
                        o3[pl.ds(i * TILE * SUB + g * lanes + v, TILE, stride=SUB), :] = o[:, v * LANE:(v + 1) * LANE]
                if q == 0:
                    w2_copy(1, 2 * g).start()
                    w2_copy(1, 2 * g + 1).start()

        def scatter(q):
            def settle(j):
                a_add(q, j)
                if j == 0:
                    h_copy(q, 0).start()
                    h_copy(q, 1).start()
                elif j == 1:
                    d_copy(q, 0, 1).start()
                elif j == 2:
                    d_copy(q, 1, 0).start()

            for j in range(chips):
                combine(q, dev(order[j], 1 - core))
                a_copy(q, j).start()
                combine(q, dev(order[j], core))
                if j > 0:
                    settle(j - 1)
            settle(chips - 1)

        def finish(q):
            for side in range(2):
                for r in range(2):
                    d_copy(q, side, r).wait_recv()
            for v in range(half_w // LANE):
                cols = slice(q * half_w + v * LANE, q * half_w + (v + 1) * LANE)
                own = accb[pl.ds((q * ep + me) * rows_blk + v, tok, stride=SUB), :]
                d0 = recv_d[pl.ds(q * 2 * rows_blk + v, tok, stride=SUB), :]
                d1 = recv_d[pl.ds((q * 2 + 1) * rows_blk + v, tok, stride=SUB), :]
                out_ref[:, cols] = (x_v[:, cols].astype(F32) + (own + d0 + d1)).astype(BF16)

        down(0)
        for c in ops_in[4:8]:
            c.wait()
        scatter(0)
        down(1)
        relay(0)
        scatter(1)
        ops_in[8].wait()
        finish(0)
        relay(1)
        finish(1)
        for q in range(2):
            for j in range(chips):
                a_copy(q, j).wait_send()
            for side in range(2):
                h_copy(q, side).wait_send()
                for r in range(2):
                    d_copy(q, side, r).wait_send()

    pl.run_scoped(
        phase_two,
        pltpu.VMEM((tiles * TILE * SUB + SUB, LANE), F32),
        pltpu.VMEM(((q_max + 1) * SUB, LANE), F32),
        pltpu.VMEM((2 * ep * rows_blk + SUB, LANE), F32),
    )

    for k in range(1, parts):
        ag(k).drain()


def solution(mesh):
    ep = mesh.shape["ep"]

    def device_step(tokens, expert_ids, norm_gain, w_router, w_gate, w_up, w_down):
        tok, top_k = expert_ids.shape
        width = tokens.shape[1]
        e_local, _, ff = w_gate.shape
        pairs = tok * top_k
        send_max = 2 * pairs // ep
        recv_max = 3 * pairs // 2
        tiles = (recv_max + e_local * (TILE - 1)) // TILE
        part_w = ff // 2
        chips = ep // 2
        rows_blk = tok * SUB
        vm = pl.BlockSpec(memory_space=pltpu.VMEM)
        hbm = pl.BlockSpec(memory_space=pl.ANY)
        dma = pltpu.SemaphoreType.DMA
        i32 = jnp.int32
        groups = (ep * send_max // LANE, LANE)
        u0, u1, slot, src, first, last, te, gate = pl.pallas_call(
            functools.partial(plan_kernel, ep, tiles),
            out_shape=[
                jax.ShapeDtypeStruct((ep * tok, part_w), BF16),
                jax.ShapeDtypeStruct((width // part_w - 1, tok, part_w), BF16),
                jax.ShapeDtypeStruct((e_local, SUB, ep * tok), F32),
                jax.ShapeDtypeStruct(groups, i32),
                jax.ShapeDtypeStruct(groups, i32),
                jax.ShapeDtypeStruct((ep, tok), i32),
                jax.ShapeDtypeStruct((1, LANE), i32),
                jax.ShapeDtypeStruct(groups, F32),
            ],
            in_specs=[hbm] * 4,
            out_specs=[vm] * 8,
            scratch_shapes=[
                pltpu.VMEM((tok, width), BF16),
                pltpu.VMEM((top_k, tok), i32),
                pltpu.VMEM((width,), BF16),
                pltpu.VMEM((w_router.shape[1], width), BF16),
                pltpu.VMEM((w_router.shape[1], tok), F32),
                pltpu.VMEM((ep, top_k, tok), i32),
                pltpu.VMEM((ep, e_local, tok), F32),
                dma((4,)),
                dma((2, ep)),
                dma((2, ep)),
                dma((14,)),
                dma((14,)),
            ],
            compiler_params=pltpu.CompilerParams(collective_id=0, has_side_effects=True),
            name="moe_plan",
        )(tokens, expert_ids.T, norm_gain, w_router.T)
        return pl.pallas_call(
            functools.partial(moe_kernel, ep, tiles),
            out_shape=jax.ShapeDtypeStruct((tok, width), BF16),
            in_specs=[hbm] * 12,
            out_specs=vm,
            scratch_shapes=[
                pltpu.SMEM((1, LANE), i32),
                pltpu.SMEM((ep * send_max,), i32),
                pltpu.SMEM((ep * send_max,), i32),
                pltpu.SMEM((ep * tok,), i32),
                pltpu.SMEM((ep * send_max,), F32),
                pltpu.VMEM((width // part_w - 1, tok, part_w), BF16),
                pltpu.VMEM((e_local, SUB, ep * tok), F32),
                pltpu.VMEM((width // part_w, ep * tok, part_w), BF16),
                pltpu.VMEM((tok, width), BF16),
                pltpu.VMEM((tiles * TILE, ff), BF16),
                *[pltpu.VMEM((e_local, part_w, part_w), BF16)] * 4,
                pltpu.VMEM((2 * chips * rows_blk, LANE), F32),
                pltpu.VMEM((2 * rows_blk, LANE), F32),
                pltpu.VMEM((4 * rows_blk + SUB, LANE), F32),
                dma((9,)),
                dma((4,)),
                dma((width // part_w, 14)),
                dma((width // part_w, 14)),
                dma((2, chips)),
                dma((2, chips)),
                dma((2, 2)),
                dma((2, 2)),
                dma((2, 4)),
                dma((2, 4)),
            ],
            compiler_params=pltpu.CompilerParams(
                collective_id=1, has_side_effects=True, vmem_limit_bytes=67_043_328),
            name="moe_block",
        )(te, src.reshape(-1), first.reshape(-1), last.reshape(-1), gate.reshape(-1), u0, u1, slot, tokens, w_gate, w_up, w_down)

    row_spec = P(("dp", "ep"), None)
    expert_spec = P("ep", None, None)
    return jax.shard_map(
        device_step, mesh=mesh,
        in_specs=(row_spec, row_spec, P(None), P(None, None), expert_spec, expert_spec, expert_spec),
        out_specs=row_spec, check_vma=False)
```
